512 devices in a mesh: band: 16 (over y, z_lo), ga: 32 (over x, z_hi, core).
Axes of the slice: x: 4, y: 8, z: 8 (z_hi: 4, z_lo: 2; z = z_hi * 2 + z_lo), core: 2. Of those that a mesh axis runs over, the one named last changes fastest.
Arguments:
- orbitals: bfloat16 [32768, 4096], P('ga', 'band'), may hold values from -6 to 6
Outputs:
- margin: float32 [4096, 4096], P('band', 'ga')
- corrected: bfloat16 [32768, 4096], P('ga', 'band')
The draws below stay inside these ranges and needn't reach their ends.
All inputs are finite; a program needn't handle non-finite values.
Results may differ from the reference program's by a relative error of at most 0.0056.
Values may be sent and summed in bfloat16 or wider, within the bound.
A program may use at most 64 MiB of HBM per device.

```python
import jax
import jax.numpy as jnp
from jax import lax

NB = 4096
NG = 32768


def draw_orbitals(key, part):
    first = jax.random.fold_in(key, 0)
    values = jnp.clip(jax.random.normal(first, (NG, NB), jnp.float32), -6.0, 6.0)
    return values.astype(jnp.bfloat16)


def setup_inputs(seed: int = 0) -> dict:
    streams_of = jax.random.split(jax.random.key(seed), 2)
    orbitals = draw_orbitals(jax.random.fold_in(streams_of[1], 71), 0)
    return dict(orbitals=orbitals)


def reference(orbitals):
    margin = jnp.dot(orbitals.T, orbitals, preferred_element_type=jnp.float32) / NG
    identity = jnp.eye(NB, dtype=jnp.float32)
    deviation = margin - identity
    square = jnp.dot(deviation, deviation, precision=lax.Precision.HIGHEST, preferred_element_type=jnp.float32)
    correction = (identity - 0.5 * deviation + 0.375 * square).astype(jnp.bfloat16)
    corrected = jnp.dot(orbitals, correction, preferred_element_type=jnp.float32).astype(jnp.bfloat16)
    return (margin, corrected)
```

```python
import jax
import jax.numpy as jnp
from jax import lax
from jax.experimental import pallas as pl
from jax.experimental.pallas import tpu as pltpu
from jax.sharding import Mesh
from jax.sharding import PartitionSpec as P

AXES = ("y", "zl", "x", "zh", "c")
NY, NX, NZ = 8, 4, 8
SLOT = (0, 1, 7, 2, 6, 3, 5, 4)
POS = tuple(SLOT.index(k) for k in range(NY))
GROUPS = ((0, 3), (3, 2), (5, 2), (7, 1))
MESH_ID = pl.DeviceIdType.MESH
F32 = jnp.float32
BF16 = jnp.bfloat16


def dot(a, b, dims=(((1,), (0,)), ((), ()))):
    return lax.dot_general(a, b, dims, preferred_element_type=F32)


def kernel(
    total_rows, x_hbm, m_out, o_out, xa, ph, xs, xr, zs, zr, db, d32, dj, da, dbb, cb, ca, cbb,
    ms, mr, acc, osb, in_sem, sw_s, sw_r, ring_s, ring_r, sib_s, sib_r, x_s, x_r, z_s, z_r,
    y_s, y_r, yf_s, yf_r, ax_s, ax_r, az_s, az_r, bz_s, bz_r, bx_s, bx_r, m_s, m_r, out_s, out_r,
):
    y = lax.axis_index("y")
    zl = lax.axis_index("zl")
    x = lax.axis_index("x")
    zh = lax.axis_index("zh")
    c = lax.axis_index("c")
    z = zh * 2 + zl
    half = ph.shape[0]
    band = ph.shape[1]
    xrows = xs.shape[2]
    zrows = zs.shape[2]
    sends = []

    def zdev(d):
        t = lax.rem(z + d + NZ, NZ)
        return {"zh": t // 2, "zl": lax.rem(t, 2)}

    def ydev(d):
        return {"y": lax.rem(y + d + NY, NY)}

    def xdev(d):
        return {"x": lax.rem(x + d + NX, NX)}

    sibling = {"c": 1 - c}

    def copy(src, dst, ssem, rsem, dev):
        return pltpu.make_async_remote_copy(
            src_ref=src, dst_ref=dst, send_sem=ssem, recv_sem=rsem, device_id=dev, device_id_type=MESH_ID
        )

    def send(src, dst, ssem, rsem, dev):
        h = copy(src, dst, ssem, rsem, dev)
        h.start()
        sends.append(h)

    def arrived(dst, ssem, rsem):
        copy(dst, dst, ssem, rsem, sibling).wait_recv()

    own_in = pltpu.make_async_copy(x_hbm.at[pl.ds(zl * half, half), :], xa.at[0, c, zl], in_sem.at[0])
    oth_in = pltpu.make_async_copy(x_hbm.at[pl.ds((1 - zl) * half, half), :], ph, in_sem.at[1])
    own_in.start()
    oth_in.start()

    barrier = pltpu.get_barrier_semaphore()
    peers = [sibling, {"zl": 1 - zl, "c": 1 - c}]
    peers += [ydev(d) for d in range(1, NY)]
    peers += [xdev(d) for d in range(1, NX)]
    peers += [zdev(d) for d in range(1, NZ)]
    for dev in peers:
        pl.semaphore_signal(barrier, inc=1, device_id=dev, device_id_type=MESH_ID)
    pl.semaphore_wait(barrier, len(peers))

    oth_in.wait()
    own_in.wait()
    send(ph, xa.at[0, c, zl], sw_s, sw_r, {"zl": 1 - zl})

    subs = (zl, 1 - zl)

    def to_minus(k, j):
        t = xa.at[k, c, subs[j]]
        u = xa.at[k + 1, c, subs[j]]
        send(t, u, ring_s.at[0, k, j], ring_r.at[0, k, j], ydev(-1))

    def to_plus(k, j):
        t = xa.at[(NY - k) % NY, c, subs[j]]
        u = xa.at[NY - k - 1, c, subs[j]]
        send(t, u, ring_s.at[1, k, j], ring_r.at[1, k, j], ydev(1))

    def to_sibling(k, j):
        t = xa.at[k, c, subs[j]]
        send(t, t, sib_s.at[k, j], sib_r.at[k, j], sibling)

    def from_sibling(k):
        for j in range(2):
            arrived(xa.at[k, 1 - c, subs[j]], sib_s.at[k, j], sib_r.at[k, j])

    def partial_margin(g):
        off, n = GROUPS[g]
        for p in range(off, off + n):
            k = SLOT[p]
            for s in range(2):
                v = dot(xa[k, 0, s], xa[0, 0, c], (((0,), (0,)), ((), ())))
                v = v + dot(xa[k, 1, s], xa[0, 1, c], (((0,), (0,)), ((), ())))
                v = v.astype(BF16)
                xs[2 * s, p] = v[:xrows]
                xs[2 * s + 1, p] = v[xrows:]
        for d in range(1, NX):
            dev = xdev(d)
            send(
                xs.at[dev["x"], pl.ds(off, n)], xr.at[d - 1, pl.ds(off, n)],
                x_s.at[g, d - 1], x_r.at[g, d - 1], dev,
            )

    def sum_over_x(g):
        off, n = GROUPS[g]
        for d in range(1, NX):
            arrived(xr.at[d - 1, pl.ds(off, n)], x_s.at[g, d - 1], x_r.at[g, d - 1])
        for p in range(off, off + n):
            v = xs[x, p].astype(F32)
            for d in range(1, NX):
                v = v + xr[d - 1, p].astype(F32)
            zs[:, p] = v.astype(BF16).reshape(NZ, zrows, band)
        for d in range(1, NZ):
            t = lax.rem(z + d, NZ)
            send(
                zs.at[t, pl.ds(off, n)], zr.at[d - 1, pl.ds(off, n)],
                z_s.at[g, d - 1], z_r.at[g, d - 1], zdev(d),
            )

    def sum_over_z(g):
        off, n = GROUPS[g]
        for d in range(1, NZ):
            arrived(zr.at[d - 1, pl.ds(off, n)], z_s.at[g, d - 1], z_r.at[g, d - 1])
        for p in range(off, off + n):
            v = zs[z, p].astype(F32)
            for d in range(1, NZ):
                v = v + zr[d - 1, p].astype(F32)
            v = v * (1.0 / total_rows)
            if p == 0:
                v = v - unit(zrows, band, x * xrows + z * zrows, c * band)
            d32[p] = v
            w = v.astype(BF16)
            db[p] = w
            put_own(da, dbb, p, w)

    def unit(rows, cols, row0, col0):
        i = lax.broadcasted_iota(jnp.int32, (rows, cols), 0) + row0
        j = lax.broadcasted_iota(jnp.int32, (rows, cols), 1) + col0
        return (i == j).astype(F32)

    def put_own(a, b, p, w):
        if p < 4:
            a[z, x, p] = w
        else:
            b[x, z, p - 4] = w

    for j in range(2):
        if j == 1:
            arrived(xa.at[0, c, 1 - zl], sw_s, sw_r)
        to_minus(0, j)
        to_plus(0, j)
        to_sibling(0, j)
    for h in range(1, 5):
        for j in range(2):
            if h < 4 or j == 0:
                arrived(xa.at[h, c, subs[j]], ring_s.at[0, h - 1, j], ring_r.at[0, h - 1, j])
                if h < 3 or (h == 3 and j == 0):
                    to_minus(h, j)
                to_sibling(h, j)
            if h < 4 or j == 1:
                arrived(xa.at[NY - h, c, subs[j]], ring_s.at[1, h - 1, j], ring_r.at[1, h - 1, j])
                if h < 3 or (h == 3 and j == 1):
                    to_plus(h, j)
                to_sibling(NY - h, j)
        if h == 1:
            from_sibling(0)
        from_sibling(h)
        if h < 4:
            from_sibling(NY - h)
        partial_margin(h - 1)
        if h > 1:
            sum_over_x(h - 2)
        if h > 2:
            sum_over_z(h - 3)
    sum_over_x(3)
    sum_over_z(2)
    sum_over_z(3)

    def plane_gather(q, a, b, between, a_done):
        def az(i, h):
            t = lax.rem(z + (h if i == 0 else NZ - h), NZ)
            if h < 4:
                return a.at[t]
            return a.at[t, pl.ds(2 * i, 2)]

        def bz(i, h):
            t = lax.rem(z + (h if i == 0 else NZ - h), NZ)
            if h < 4:
                return b.at[x, t]
            return b.at[x, t, pl.ds(2 * i, 2)]

        def ring(blk, i, h, ss, rs):
            t = lax.rem(z + (h - 1 if i == 0 else NZ - h + 1), NZ)
            if blk == 0:
                v = a.at[t] if h < 4 else a.at[t, pl.ds(2 * i, 2)]
            else:
                v = b.at[x, t] if h < 4 else b.at[x, t, pl.ds(2 * i, 2)]
            send(v, v, ss.at[q, i, h - 1], rs.at[q, i, h - 1], zdev(-1 if i == 0 else 1))

        for d in range(1, NX):
            send(a.at[z, x], a.at[z, x], ax_s.at[q, d - 1], ax_r.at[q, d - 1], xdev(d))
        for i in range(2):
            ring(1, i, 1, bz_s, bz_r)

        def b_hop(h):
            for i in range(2):
                arrived(bz(i, h), bz_s.at[q, i, h - 1], bz_r.at[q, i, h - 1])
                if h < 4:
                    ring(1, i, h + 1, bz_s, bz_r)

        def a_hop(h):
            for i in range(2):
                arrived(az(i, h), az_s.at[q, i, h - 1], az_r.at[q, i, h - 1])
                if h < 4:
                    ring(0, i, h + 1, az_s, az_r)

        b_hop(1)
        for d in range(1, NX):
            t = lax.rem(x + NX - d, NX)
            arrived(a.at[z, t], ax_s.at[q, d - 1], ax_r.at[q, d - 1])
        for i in range(2):
            ring(0, i, 1, az_s, az_r)
        b_hop(2)
        b_hop(3)
        a_hop(1)
        b_hop(4)
        for i in range(2):
            send(b.at[x], b.at[x], bx_s.at[q, i, 0], bx_r.at[q, i, 0], xdev(-1 if i == 0 else 1))
        between()
        a_hop(2)
        a_hop(3)
        for i in range(2):
            t = lax.rem(x + (1 if i == 0 else NX - 1), NX)
            arrived(b.at[t], bx_s.at[q, i, 0], bx_r.at[q, i, 0])
            v = b.at[t, pl.ds(4 * i, 4)]
            send(v, v, bx_s.at[q, i, 1], bx_r.at[q, i, 1], xdev(-1 if i == 0 else 1))
        a_hop(4)
        a_done()
        for i in range(2):
            t = lax.rem(x + 2, NX)
            arrived(b.at[t, pl.ds(4 * i, 4)], bx_s.at[q, i, 1], bx_r.at[q, i, 1])

    dj[0, c] = db[...].reshape(NY * zrows, band)
    send(dj.at[0, c], dj.at[0, c], yf_s.at[0], yf_r.at[0], sibling)
    for k in range(1, NY):
        send(dj.at[0, c], dj.at[k, c], y_s.at[k - 1], y_r.at[k - 1], ydev(-k))

    def pass_on():
        for k in range(1, NY):
            arrived(dj.at[k, c], y_s.at[k - 1], y_r.at[k - 1])
            send(dj.at[k, c], dj.at[k, c], yf_s.at[k], yf_r.at[k], sibling)

    plane_gather(0, da, dbb, pass_on, lambda: None)
    for k in range(NY):
        arrived(dj.at[k, 1 - c], yf_s.at[k], yf_r.at[k])

    def quarter(a, b, p, q):
        v = a[:, q, p] if p < 4 else b[q, :, p - 4]
        return v.reshape(xrows, band)

    def rows_of(a, b, p, s):
        return jnp.concatenate([quarter(a, b, p, 2 * s), quarter(a, b, p, 2 * s + 1)], axis=0)

    acc_sq = [None] * NY
    for k in range(NY):
        part = dot(dj[k, 0], rows_of(da, dbb, POS[k], 0)) + dot(dj[k, 1], rows_of(da, dbb, POS[k], 1))
        for p in range(NY):
            m = POS[(k + SLOT[p]) % NY]
            piece = part[p * zrows : (p + 1) * zrows]
            acc_sq[m] = piece if acc_sq[m] is None else acc_sq[m] + piece
    for p in range(NY):
        v = 0.375 * acc_sq[p] - 0.5 * d32[p]
        if p == 0:
            v = v + unit(zrows, band, x * xrows + z * zrows, c * band)
        put_own(ca, cbb, p, v.astype(BF16))

    kg = lax.rem(x * 2 + zh // 2 - y + NY, NY)
    pg = jnp.where(kg == 0, 0, jnp.where(kg <= 4, 2 * kg - 1, 2 * (NY - kg)))
    pa = jnp.minimum(pg, 3)
    pb = jnp.maximum(pg - 4, 0)

    def mirror(core):
        q = lax.rem(zh, 2) * 2 + core
        va = da[:, q, pa].reshape(xrows, band)
        vb = dbb[q, :, pb].reshape(xrows, band)
        return jnp.where(pg < 4, va.astype(F32), vb.astype(F32))

    def margin_work():
        ms[...] = mirror(1 - c).astype(BF16)
        send(ms, mr, m_s, m_r, sibling)

    def product(part):
        for cc in range(2):
            for p in range(4 * part, 4 * part + 4):
                k = SLOT[p]
                for s in range(2):
                    v = dot(xa[k, cc, s], rows_of(ca, cbb, p, s))
                    if part == 0 and p == 0 and s == 0:
                        acc[cc] = v
                    else:
                        acc[cc] += v
            if part == 1:
                osb[cc] = acc[cc].astype(BF16)
                mine = (zl == c) & (c == cc)
                to = copy(
                    osb.at[cc], o_out.at[pl.ds(zl * half, half), :], out_s.at[cc], out_r.at[zl], {"zl": c, "c": cc}
                )

                @pl.when(jnp.logical_not(mine))
                def _():
                    to.start()

                @pl.when(mine)
                def _():
                    o_out[pl.ds(pl.multiple_of(zl * half, half), half), :] = osb[cc]

    def first_half():
        arrived(mr, m_s, m_r)
        v = jnp.where(zl == c, mirror(c), mr[...].astype(F32))
        rows0 = (y * 2 + zl) * band
        cols0 = (x * 8 + zh * 2 + c) * xrows
        m_out[...] = v.T + unit(band, xrows, rows0, cols0)
        product(0)

    plane_gather(1, ca, cbb, margin_work, first_half)
    product(1)

    other = o_out.at[pl.ds((1 - zl) * half, half), :]
    arrived(other, out_s.at[0], out_r.at[1 - zl])

    @pl.when(zl != c)
    def _():
        arrived(o_out.at[pl.ds(zl * half, half), :], out_s.at[0], out_r.at[zl])

    for cc in range(2):

        @pl.when(jnp.logical_not((zl == c) & (c == cc)))
        def _():
            copy(
                osb.at[cc], o_out.at[pl.ds(zl * half, half), :], out_s.at[cc], out_r.at[zl], {"zl": c, "c": cc}
            ).wait_send()

    for h in sends:
        h.wait_send()


def shards(total_rows, orbitals):
    rows, band = orbitals.shape
    half = rows // 2
    xrows = 2 * band // NX
    zrows = xrows // NZ
    dma = pltpu.SemaphoreType.DMA
    v = pltpu.VMEM
    scratch = [
        v((NY, 2, 2, half, band), BF16),
        v((half, band), BF16),
        v((NX, NY, xrows, band), BF16),
        v((NX - 1, NY, xrows, band), BF16),
        v((NZ, NY, zrows, band), BF16),
        v((NZ - 1, NY, zrows, band), BF16),
        v((NY, zrows, band), BF16),
        v((NY, zrows, band), F32),
        v((NY, 2, NY * zrows, band), BF16),
        v((NZ, NX, 4, zrows, band), BF16),
        v((NX, NZ, 4, zrows, band), BF16),
        v((NY, zrows, band), BF16),
        v((NZ, NX, 4, zrows, band), BF16),
        v((NX, NZ, 4, zrows, band), BF16),
        v((xrows, band), BF16),
        v((xrows, band), BF16),
        v((2, half, band), F32),
        v((2, half, band), BF16),
        dma((2,)),
        dma, dma,
        dma((2, 4, 2)), dma((2, 4, 2)),
        dma((NY, 2)), dma((NY, 2)),
        dma((4, NX - 1)), dma((4, NX - 1)),
        dma((4, NZ - 1)), dma((4, NZ - 1)),
        dma((NY - 1,)), dma((NY - 1,)),
        dma((NY,)), dma((NY,)),
        dma((2, NX - 1)), dma((2, NX - 1)),
        dma((2, 2, 4)), dma((2, 2, 4)),
        dma((2, 2, 4)), dma((2, 2, 4)),
        dma((2, 2, 2)), dma((2, 2, 2)),
        dma, dma,
        dma((2,)), dma((2,)),
    ]

    def body(*refs):
        kernel(total_rows, *refs)

    return pl.pallas_call(
        body,
        out_shape=(
            jax.ShapeDtypeStruct((band, xrows), F32),
            jax.ShapeDtypeStruct((rows, band), BF16),
        ),
        in_specs=[pl.BlockSpec(memory_space=pl.ANY)],
        out_specs=(pl.BlockSpec(memory_space=pltpu.VMEM), pl.BlockSpec(memory_space=pltpu.VMEM)),
        scratch_shapes=scratch,
        compiler_params=pltpu.CompilerParams(
            collective_id=0, has_side_effects=True, vmem_limit_bytes=56 * 1024 * 1024
        ),
    )(orbitals)


def solution(mesh):
    finer = Mesh(mesh.devices.reshape(NY, 2, NX, NZ // 2, 2), AXES)
    coeffs = ("x", "zh", "c")
    bands = ("y", "zl")

    def run(orbitals):
        total = orbitals.shape[0]
        return jax.shard_map(
            lambda o: shards(total, o),
            mesh=finer,
            in_specs=(P(coeffs, bands),),
            out_specs=(P(bands, coeffs), P(coeffs, bands)),
            check_vma=False,
        )(orbitals)

    return run
```

```python
import jax
import jax.numpy as jnp
from jax import lax
from jax.experimental import pallas as pl
from jax.experimental.pallas import tpu as pltpu
from jax.sharding import Mesh
from jax.sharding import PartitionSpec as P

AXES = ("y", "zl", "x", "zh", "c")
NY, NX, NZ = 8, 4, 8
SLOT = (0, 1, 7, 2, 6, 3, 5, 4)
POS = tuple(SLOT.index(k) for k in range(NY))
GROUPS = ((0, 3), (3, 2), (5, 2), (7, 1))
MESH_ID = pl.DeviceIdType.MESH
F32 = jnp.float32
BF16 = jnp.bfloat16


def dot(a, b, dims=(((1,), (0,)), ((), ()))):
    return lax.dot_general(a, b, dims, preferred_element_type=F32)


def kernel(
    total_rows, x_hbm, m_out, o_out, xa, ph, xs, xr, zs, zr, db, d32, dj, da, ca, cbb,
    ms, mr, acc, osb, in_sem, sw_s, sw_r, ring_s, ring_r, sib_s, sib_r, x_s, x_r, z_s, z_r,
    y_s, y_r, yf_s, yf_r, gx_s, gx_r, gz_s, gz_r, hz_s, hz_r, hx_s, hx_r,
    ax_s, ax_r, az_s, az_r, bz_s, bz_r, bx_s, bx_r, m_s, m_r, out_s, out_r,
):
    y = lax.axis_index("y")
    zl = lax.axis_index("zl")
    x = lax.axis_index("x")
    zh = lax.axis_index("zh")
    c = lax.axis_index("c")
    z = zh * 2 + zl
    half = ph.shape[0]
    band = ph.shape[1]
    xrows = xs.shape[2]
    zrows = zs.shape[2]
    sends = []

    def zdev(d):
        t = lax.rem(z + d + NZ, NZ)
        return {"zh": t // 2, "zl": lax.rem(t, 2)}

    def ydev(d):
        return {"y": lax.rem(y + d + NY, NY)}

    def xdev(d):
        return {"x": lax.rem(x + d + NX, NX)}

    sibling = {"c": 1 - c}

    def copy(src, dst, ssem, rsem, dev):
        return pltpu.make_async_remote_copy(
            src_ref=src, dst_ref=dst, send_sem=ssem, recv_sem=rsem, device_id=dev, device_id_type=MESH_ID
        )

    def send(src, dst, ssem, rsem, dev):
        h = copy(src, dst, ssem, rsem, dev)
        h.start()
        sends.append(h)

    def arrived(dst, ssem, rsem):
        copy(dst, dst, ssem, rsem, sibling).wait_recv()

    own_in = pltpu.make_async_copy(x_hbm.at[pl.ds(zl * half, half), :], xa.at[0, c, zl], in_sem.at[0])
    oth_in = pltpu.make_async_copy(x_hbm.at[pl.ds((1 - zl) * half, half), :], ph, in_sem.at[1])
    own_in.start()
    oth_in.start()

    barrier = pltpu.get_barrier_semaphore()
    peers = [sibling, {"zl": 1 - zl, "c": 1 - c}]
    peers += [ydev(d) for d in range(1, NY)]
    peers += [xdev(d) for d in range(1, NX)]
    peers += [zdev(d) for d in range(1, NZ)]
    for dev in peers:
        pl.semaphore_signal(barrier, inc=1, device_id=dev, device_id_type=MESH_ID)
    pl.semaphore_wait(barrier, len(peers))

    oth_in.wait()
    own_in.wait()
    send(ph, xa.at[0, c, zl], sw_s, sw_r, {"zl": 1 - zl})

    subs = (zl, 1 - zl)

    def to_minus(k, j):
        t = xa.at[k, c, subs[j]]
        u = xa.at[k + 1, c, subs[j]]
        send(t, u, ring_s.at[0, k, j], ring_r.at[0, k, j], ydev(-1))

    def to_plus(k, j):
        t = xa.at[(NY - k) % NY, c, subs[j]]
        u = xa.at[NY - k - 1, c, subs[j]]
        send(t, u, ring_s.at[1, k, j], ring_r.at[1, k, j], ydev(1))

    def to_sibling(k, j):
        t = xa.at[k, c, subs[j]]
        send(t, t, sib_s.at[k, j], sib_r.at[k, j], sibling)

    def from_sibling(k, j):
        arrived(xa.at[k, 1 - c, subs[j]], sib_s.at[k, j], sib_r.at[k, j])

    def partial_margin(g, j):
        off, n = GROUPS[g]
        s = subs[j]
        for p in range(off, off + n):
            k = SLOT[p]
            v = dot(xa[k, 0, s], xa[0, 0, c], (((0,), (0,)), ((), ())))
            v = v + dot(xa[k, 1, s], xa[0, 1, c], (((0,), (0,)), ((), ())))
            v = v.astype(BF16)
            xs[2 * s, p] = v[:xrows]
            xs[2 * s + 1, p] = v[xrows:]
        for i in range(2):
            to = 2 * s + i
            d = lax.rem(to - x + NX, NX)
            at = jnp.maximum(d - 1, 0)
            h = copy(xs.at[to, pl.ds(off, n)], xr.at[at, pl.ds(off, n)], x_s.at[g, at], x_r.at[g, at], {"x": to})

            @pl.when(d > 0)
            def _():
                h.start()

    def partial_sent(g):
        off, n = GROUPS[g]
        for d in range(1, NX):
            t = xr.at[d - 1, pl.ds(off, n)]
            copy(t, t, x_s.at[g, d - 1], x_r.at[g, d - 1], sibling).wait_send()

    def sum_over_x(g):
        off, n = GROUPS[g]
        for d in range(1, NX):
            arrived(xr.at[d - 1, pl.ds(off, n)], x_s.at[g, d - 1], x_r.at[g, d - 1])
        for p in range(off, off + n):
            v = xs[x, p].astype(F32)
            for d in range(1, NX):
                v = v + xr[d - 1, p].astype(F32)
            zs[:, p] = v.astype(BF16).reshape(NZ, zrows, band)
        for d in range(1, NZ):
            t = lax.rem(z + d, NZ)
            send(
                zs.at[t, pl.ds(off, n)], zr.at[d - 1, pl.ds(off, n)],
                z_s.at[g, d - 1], z_r.at[g, d - 1], zdev(d),
            )

    def sum_over_z(g):
        off, n = GROUPS[g]
        for d in range(1, NZ):
            arrived(zr.at[d - 1, pl.ds(off, n)], z_s.at[g, d - 1], z_r.at[g, d - 1])
        for p in range(off, off + n):
            v = zs[z, p].astype(F32)
            for d in range(1, NZ):
                v = v + zr[d - 1, p].astype(F32)
            v = v * (1.0 / total_rows)
            if p == 0:
                v = v - unit(zrows, band, x * xrows + z * zrows, c * band)
            d32[p] = v
            w = v.astype(BF16)
            db[p] = w
            da[p, z, x] = w

    def unit(rows, cols, row0, col0):
        i = lax.broadcasted_iota(jnp.int32, (rows, cols), 0) + row0
        j = lax.broadcasted_iota(jnp.int32, (rows, cols), 1) + col0
        return (i == j).astype(F32)

    def put_own(a, b, p, w):
        if p < 4:
            a[z, x, p] = w
        else:
            b[x, z, p - 4] = w

    for j in range(2):
        if j == 1:
            arrived(xa.at[0, c, 1 - zl], sw_s, sw_r)
        to_minus(0, j)
        to_plus(0, j)
        to_sibling(0, j)
    def ring_step(h, j):
        if h < 4 or j == 0:
            arrived(xa.at[h, c, subs[j]], ring_s.at[0, h - 1, j], ring_r.at[0, h - 1, j])
            if h < 3 or (h == 3 and j == 0):
                to_minus(h, j)
            to_sibling(h, j)
        if h < 4 or j == 1:
            arrived(xa.at[NY - h, c, subs[j]], ring_s.at[1, h - 1, j], ring_r.at[1, h - 1, j])
            if h < 3 or (h == 3 and j == 1):
                to_plus(h, j)
            to_sibling(NY - h, j)

    def use(h, j):
        if (h, j) == (1, 0):
            from_sibling(0, 0)
            from_sibling(0, 1)
        from_sibling(h, j)
        if h < 4:
            from_sibling(NY - h, j)
        partial_margin(h - 1, j)

    def gather_x(g):
        off, n = GROUPS[g]
        v = da.at[pl.ds(off, n), z, x]
        for d in range(1, NX):
            send(v, v, gx_s.at[g, d - 1], gx_r.at[g, d - 1], xdev(d))

    def slab(g, i, h):
        off, n = GROUPS[g]
        t = lax.rem(z + (h if i == 0 else NZ - h), NZ)
        return t, pl.ds(off, n)

    def hop_send(g, i, h):
        t, ps = slab(g, i, h - 1)
        v = da.at[ps, t] if h < 4 else da.at[ps, t, pl.ds(2 * i, 2)]
        send(v, v, gz_s.at[g, i, h - 1], gz_r.at[g, i, h - 1], zdev(-1 if i == 0 else 1))

    def gather_z(g):
        off, n = GROUPS[g]
        for d in range(1, NX):
            t = lax.rem(x + NX - d, NX)
            arrived(da.at[pl.ds(off, n), z, t], gx_s.at[g, d - 1], gx_r.at[g, d - 1])
        for i in range(2):
            hop_send(g, i, 1)

    def hop(g, h):
        for i in range(2):
            t, ps = slab(g, i, h)
            v = da.at[ps, t] if h < 4 else da.at[ps, t, pl.ds(2 * i, 2)]
            arrived(v, gz_s.at[g, i, h - 1], gz_r.at[g, i, h - 1])
            if h < 4:
                hop_send(g, i, h + 1)

    def near_z(g):
        off, n = GROUPS[g]
        v = da.at[pl.ds(off, n), z, x]
        for d in range(1, NZ):
            send(v, v, hz_s.at[g - 2, d - 1], hz_r.at[g - 2, d - 1], zdev(d))

    def near_x(g):
        off, n = GROUPS[g]
        for d in range(1, NZ):
            t = lax.rem(z + NZ - d, NZ)
            arrived(da.at[pl.ds(off, n), t, x], hz_s.at[g - 2, d - 1], hz_r.at[g - 2, d - 1])
        v = da.at[pl.ds(off, n), :, x]
        for d in range(1, NX):
            send(v, v, hx_s.at[g - 2, d - 1], hx_r.at[g - 2, d - 1], xdev(d))

    def near_done(g):
        off, n = GROUPS[g]
        for d in range(1, NX):
            t = lax.rem(x + NX - d, NX)
            arrived(da.at[pl.ds(off, n), :, t], hx_s.at[g - 2, d - 1], hx_r.at[g - 2, d - 1])

    PARTS = ((0, 5), (5, 3))

    def rows_part(i):
        off, n = PARTS[i]
        return pl.ds(off, n)

    def left_send(i):
        ps = rows_part(i)
        for k in range(1, NY):
            send(db.at[ps], dj.at[k, c, ps], y_s.at[i, k - 1], y_r.at[i, k - 1], ydev(-k))
        off, n = PARTS[i]
        for p in range(off, off + n):
            dj[0, c, p] = db[p]
        if i == 1:
            send(db, dj.at[0, c], yf_s.at[0], yf_r.at[0], sibling)

    def left_pass():
        for k in range(1, NY):
            for i in range(2):
                arrived(dj.at[k, c, rows_part(i)], y_s.at[i, k - 1], y_r.at[i, k - 1])
            send(dj.at[k, c], dj.at[k, c], yf_s.at[k], yf_r.at[k], sibling)

    for h in range(1, 4):
        for j in range(2):
            ring_step(h, j)
            use(h, j)
            if (h, j) == (2, 1):
                sum_over_x(0)
            if (h, j) == (3, 0):
                sum_over_x(1)
            if (h, j) == (3, 1):
                sum_over_z(0)
                gather_x(0)
    ring_step(4, 0)
    ring_step(4, 1)
    gather_z(0)
    use(4, 0)
    use(4, 1)
    sum_over_x(2)
    sum_over_z(1)
    gather_x(1)
    left_send(0)
    hop(0, 1)
    sum_over_x(3)
    gather_z(1)
    sum_over_z(2)
    near_z(2)
    hop(0, 2)
    sum_over_z(3)
    near_z(3)
    left_send(1)
    hop(1, 1)
    hop(0, 3)
    hop(1, 2)
    near_x(2)
    hop(0, 4)
    hop(1, 3)
    near_x(3)
    left_pass()
    hop(1, 4)
    near_done(2)
    near_done(3)
    for k in range(NY):
        arrived(dj.at[k, 1 - c], yf_s.at[k], yf_r.at[k])

    def plane_gather(a, b, between, a_done):
        def az(i, h):
            t = lax.rem(z + (h if i == 0 else NZ - h), NZ)
            if h < 4:
                return a.at[t]
            return a.at[t, pl.ds(2 * i, 2)]

        def bz(i, h):
            t = lax.rem(z + (h if i == 0 else NZ - h), NZ)
            if h < 4:
                return b.at[x, t]
            return b.at[x, t, pl.ds(2 * i, 2)]

        def ring(blk, i, h, ss, rs):
            t = lax.rem(z + (h - 1 if i == 0 else NZ - h + 1), NZ)
            if blk == 0:
                v = a.at[t] if h < 4 else a.at[t, pl.ds(2 * i, 2)]
            else:
                v = b.at[x, t] if h < 4 else b.at[x, t, pl.ds(2 * i, 2)]
            send(v, v, ss.at[i, h - 1], rs.at[i, h - 1], zdev(-1 if i == 0 else 1))

        for d in range(1, NX):
            send(a.at[z, x], a.at[z, x], ax_s.at[d - 1], ax_r.at[d - 1], xdev(d))
        for i in range(2):
            ring(1, i, 1, bz_s, bz_r)

        def b_hop(h):
            for i in range(2):
                arrived(bz(i, h), bz_s.at[i, h - 1], bz_r.at[i, h - 1])
                if h < 4:
                    ring(1, i, h + 1, bz_s, bz_r)

        def a_hop(h):
            for i in range(2):
                arrived(az(i, h), az_s.at[i, h - 1], az_r.at[i, h - 1])
                if h < 4:
                    ring(0, i, h + 1, az_s, az_r)

        b_hop(1)
        for d in range(1, NX):
            t = lax.rem(x + NX - d, NX)
            arrived(a.at[z, t], ax_s.at[d - 1], ax_r.at[d - 1])
        for i in range(2):
            ring(0, i, 1, az_s, az_r)
        b_hop(2)
        b_hop(3)
        a_hop(1)
        b_hop(4)
        for i in range(2):
            send(b.at[x], b.at[x], bx_s.at[i, 0], bx_r.at[i, 0], xdev(-1 if i == 0 else 1))
        between()
        a_hop(2)
        a_hop(3)
        for i in range(2):
            t = lax.rem(x + (1 if i == 0 else NX - 1), NX)
            arrived(b.at[t], bx_s.at[i, 0], bx_r.at[i, 0])
            v = b.at[t, pl.ds(4 * i, 4)]
            send(v, v, bx_s.at[i, 1], bx_r.at[i, 1], xdev(-1 if i == 0 else 1))
        a_hop(4)
        a_done()
        for i in range(2):
            t = lax.rem(x + 2, NX)
            arrived(b.at[t, pl.ds(4 * i, 4)], bx_s.at[i, 1], bx_r.at[i, 1])

    def quarter(a, b, p, q):
        v = a[:, q, p] if p < 4 else b[q, :, p - 4]
        return v.reshape(xrows, band)

    def rows_of(a, b, p, s):
        return jnp.concatenate([quarter(a, b, p, 2 * s), quarter(a, b, p, 2 * s + 1)], axis=0)

    def dev_rows(p, s):
        return jnp.concatenate([da[p, :, 2 * s + i].reshape(xrows, band) for i in range(2)], axis=0)

    acc_sq = [None] * NY
    for k in range(NY):
        left = [dj[k, s].reshape(NY * zrows, band) for s in range(2)]
        part = dot(left[0], dev_rows(POS[k], 0)) + dot(left[1], dev_rows(POS[k], 1))
        for p in range(NY):
            m = POS[(k + SLOT[p]) % NY]
            piece = part[p * zrows : (p + 1) * zrows]
            acc_sq[m] = piece if acc_sq[m] is None else acc_sq[m] + piece
    for p in range(NY):
        v = 0.375 * acc_sq[p] - 0.5 * d32[p]
        if p == 0:
            v = v + unit(zrows, band, x * xrows + z * zrows, c * band)
        put_own(ca, cbb, p, v.astype(BF16))

    kg = lax.rem(x * 2 + zh // 2 - y + NY, NY)
    pg = jnp.where(kg == 0, 0, jnp.where(kg <= 4, 2 * kg - 1, 2 * (NY - kg)))

    def mirror(core):
        q = lax.rem(zh, 2) * 2 + core
        return da[pg, :, q].reshape(xrows, band).astype(F32)

    def margin_work():
        ms[...] = mirror(1 - c).astype(BF16)
        send(ms, mr, m_s, m_r, sibling)

    def product(part):
        for cc in range(2):
            for p in range(4 * part, 4 * part + 4):
                k = SLOT[p]
                for s in range(2):
                    v = dot(xa[k, cc, s], rows_of(ca, cbb, p, s))
                    if part == 0 and p == 0 and s == 0:
                        acc[cc] = v
                    else:
                        acc[cc] += v
            if part == 1:
                osb[cc] = acc[cc].astype(BF16)
                mine = (zl == c) & (c == cc)
                to = copy(
                    osb.at[cc], o_out.at[pl.ds(zl * half, half), :], out_s.at[cc], out_r.at[zl], {"zl": c, "c": cc}
                )

                @pl.when(jnp.logical_not(mine))
                def _():
                    to.start()

                @pl.when(mine)
                def _():
                    o_out[pl.ds(pl.multiple_of(zl * half, half), half), :] = osb[cc]

    def first_half():
        arrived(mr, m_s, m_r)
        v = jnp.where(zl == c, mirror(c), mr[...].astype(F32))
        rows0 = (y * 2 + zl) * band
        cols0 = (x * 8 + zh * 2 + c) * xrows
        m_out[...] = v.T + unit(band, xrows, rows0, cols0)
        product(0)

    plane_gather(ca, cbb, margin_work, first_half)
    product(1)

    other = o_out.at[pl.ds((1 - zl) * half, half), :]
    arrived(other, out_s.at[0], out_r.at[1 - zl])

    @pl.when(zl != c)
    def _():
        arrived(o_out.at[pl.ds(zl * half, half), :], out_s.at[0], out_r.at[zl])

    for cc in range(2):

        @pl.when(jnp.logical_not((zl == c) & (c == cc)))
        def _():
            copy(
                osb.at[cc], o_out.at[pl.ds(zl * half, half), :], out_s.at[cc], out_r.at[zl], {"zl": c, "c": cc}
            ).wait_send()

    for g in range(len(GROUPS)):
        partial_sent(g)
    for h in sends:
        h.wait_send()


def shards(total_rows, orbitals):
    rows, band = orbitals.shape
    half = rows // 2
    xrows = 2 * band // NX
    zrows = xrows // NZ
    dma = pltpu.SemaphoreType.DMA
    v = pltpu.VMEM
    scratch = [
        v((NY, 2, 2, half, band), BF16),
        v((half, band), BF16),
        v((NX, NY, xrows, band), BF16),
        v((NX - 1, NY, xrows, band), BF16),
        v((NZ, NY, zrows, band), BF16),
        v((NZ - 1, NY, zrows, band), BF16),
        v((NY, zrows, band), BF16),
        v((NY, zrows, band), F32),
        v((NY, 2, NY, zrows, band), BF16),
        v((NY, NZ, NX, zrows, band), BF16),
        v((NZ, NX, 4, zrows, band), BF16),
        v((NX, NZ, 4, zrows, band), BF16),
        v((xrows, band), BF16),
        v((xrows, band), BF16),
        v((2, half, band), F32),
        v((2, half, band), BF16),
        dma((2,)),
        dma, dma,
        dma((2, 4, 2)), dma((2, 4, 2)),
        dma((NY, 2)), dma((NY, 2)),
        dma((4, NX - 1)), dma((4, NX - 1)),
        dma((4, NZ - 1)), dma((4, NZ - 1)),
        dma((2, NY - 1)), dma((2, NY - 1)),
        dma((NY,)), dma((NY,)),
        dma((2, NX - 1)), dma((2, NX - 1)),
        dma((2, 2, 4)), dma((2, 2, 4)),
        dma((2, NZ - 1)), dma((2, NZ - 1)),
        dma((2, NX - 1)), dma((2, NX - 1)),
        dma((NX - 1,)), dma((NX - 1,)),
        dma((2, 4)), dma((2, 4)),
        dma((2, 4)), dma((2, 4)),
        dma((2, 2)), dma((2, 2)),
        dma, dma,
        dma((2,)), dma((2,)),
    ]

    def body(*refs):
        kernel(total_rows, *refs)

    return pl.pallas_call(
        body,
        out_shape=(
            jax.ShapeDtypeStruct((band, xrows), F32),
            jax.ShapeDtypeStruct((rows, band), BF16),
        ),
        in_specs=[pl.BlockSpec(memory_space=pl.ANY)],
        out_specs=(pl.BlockSpec(memory_space=pltpu.VMEM), pl.BlockSpec(memory_space=pltpu.VMEM)),
        scratch_shapes=scratch,
        compiler_params=pltpu.CompilerParams(
            collective_id=0, has_side_effects=True, vmem_limit_bytes=56 * 1024 * 1024
        ),
    )(orbitals)


def solution(mesh):
    finer = Mesh(mesh.devices.reshape(NY, 2, NX, NZ // 2, 2), AXES)
    coeffs = ("x", "zh", "c")
    bands = ("y", "zl")

    def run(orbitals):
        total = orbitals.shape[0]
        return jax.shard_map(
            lambda o: shards(total, o),
            mesh=finer,
            in_specs=(P(coeffs, bands),),
            out_specs=(P(bands, coeffs), P(coeffs, bands)),
            check_vma=False,
        )(orbitals)

    return run
```

```python
import jax
import jax.numpy as jnp
from jax import lax
from jax.experimental import pallas as pl
from jax.experimental.pallas import tpu as pltpu
from jax.sharding import Mesh
from jax.sharding import PartitionSpec as P

AXES = ("y", "zl", "x", "zh", "c")
NY, NX, NZ = 8, 4, 8
SLOT = (0, 1, 7, 2, 6, 3, 5, 4)
POS = tuple(SLOT.index(k) for k in range(NY))
GROUPS = ((0, 3), (3, 2), (5, 2), (7, 1))
MESH_ID = pl.DeviceIdType.MESH
F32 = jnp.float32
BF16 = jnp.bfloat16


def dot(a, b, dims=(((1,), (0,)), ((), ()))):
    return lax.dot_general(a, b, dims, preferred_element_type=F32)


def kernel(
    total_rows, x_hbm, m_out, o_out, xa, ph, xs, xr, zs, zr, db, d32, dj, da, ca,
    ms, mr, acc, osb, in_sem, sw_s, sw_r, ring_s, ring_r, sib_s, sib_r, x_s, x_r, z_s, z_r,
    y_s, y_r, yf_s, yf_r, gx_s, gx_r, gz_s, gz_r, hz_s, hz_r, hx_s, hx_r,
    ax_s, ax_r, az_s, az_r, bz_s, bz_r, bx_s, bx_r, m_s, m_r, out_s, out_r,
):
    y = lax.axis_index("y")
    zl = lax.axis_index("zl")
    x = lax.axis_index("x")
    zh = lax.axis_index("zh")
    c = lax.axis_index("c")
    z = zh * 2 + zl
    half = ph.shape[0]
    band = ph.shape[1]
    xrows = xs.shape[2]
    zrows = zs.shape[2]
    sends = []

    def zdev(d):
        t = lax.rem(z + d + NZ, NZ)
        return {"zh": t // 2, "zl": lax.rem(t, 2)}

    def ydev(d):
        return {"y": lax.rem(y + d + NY, NY)}

    def xdev(d):
        return {"x": lax.rem(x + d + NX, NX)}

    sibling = {"c": 1 - c}

    def copy(src, dst, ssem, rsem, dev):
        return pltpu.make_async_remote_copy(
            src_ref=src, dst_ref=dst, send_sem=ssem, recv_sem=rsem, device_id=dev, device_id_type=MESH_ID
        )

    def send(src, dst, ssem, rsem, dev):
        h = copy(src, dst, ssem, rsem, dev)
        h.start()
        sends.append(h)

    def arrived(dst, ssem, rsem):
        copy(dst, dst, ssem, rsem, sibling).wait_recv()

    own_in = pltpu.make_async_copy(x_hbm.at[pl.ds(zl * half, half), :], xa.at[0, c, zl], in_sem.at[0])
    oth_in = pltpu.make_async_copy(x_hbm.at[pl.ds((1 - zl) * half, half), :], ph, in_sem.at[1])
    own_in.start()
    oth_in.start()

    barrier = pltpu.get_barrier_semaphore()
    peers = [sibling, {"zl": 1 - zl, "c": 1 - c}]
    peers += [ydev(d) for d in range(1, NY)]
    peers += [xdev(d) for d in range(1, NX)]
    peers += [zdev(d) for d in range(1, NZ)]
    for dev in peers:
        pl.semaphore_signal(barrier, inc=1, device_id=dev, device_id_type=MESH_ID)
    pl.semaphore_wait(barrier, len(peers))

    oth_in.wait()
    own_in.wait()
    send(ph, xa.at[0, c, zl], sw_s, sw_r, {"zl": 1 - zl})

    subs = (zl, 1 - zl)

    def to_minus(k, j):
        t = xa.at[k, c, subs[j]]
        u = xa.at[k + 1, c, subs[j]]
        send(t, u, ring_s.at[0, k, j], ring_r.at[0, k, j], ydev(-1))

    def to_plus(k, j):
        t = xa.at[(NY - k) % NY, c, subs[j]]
        u = xa.at[NY - k - 1, c, subs[j]]
        send(t, u, ring_s.at[1, k, j], ring_r.at[1, k, j], ydev(1))

    def to_sibling(k, j):
        t = xa.at[k, c, subs[j]]
        send(t, t, sib_s.at[k, j], sib_r.at[k, j], sibling)

    def from_sibling(k, j):
        arrived(xa.at[k, 1 - c, subs[j]], sib_s.at[k, j], sib_r.at[k, j])

    def partial_margin(g, j):
        off, n = GROUPS[g]
        s = subs[j]
        for p in range(off, off + n):
            k = SLOT[p]
            v = dot(xa[k, 0, s], xa[0, 0, c], (((0,), (0,)), ((), ())))
            v = v + dot(xa[k, 1, s], xa[0, 1, c], (((0,), (0,)), ((), ())))
            v = v.astype(BF16)
            xs[2 * s, p] = v[:xrows]
            xs[2 * s + 1, p] = v[xrows:]
        for i in range(2):
            to = 2 * s + i
            d = lax.rem(to - x + NX, NX)
            at = jnp.maximum(d - 1, 0)
            h = copy(xs.at[to, pl.ds(off, n)], xr.at[at, pl.ds(off, n)], x_s.at[g, at], x_r.at[g, at], {"x": to})

            @pl.when(d > 0)
            def _():
                h.start()

    def partial_sent(g):
        off, n = GROUPS[g]
        for d in range(1, NX):
            t = xr.at[d - 1, pl.ds(off, n)]
            copy(t, t, x_s.at[g, d - 1], x_r.at[g, d - 1], sibling).wait_send()

    def sum_over_x(g):
        off, n = GROUPS[g]
        for d in range(1, NX):
            arrived(xr.at[d - 1, pl.ds(off, n)], x_s.at[g, d - 1], x_r.at[g, d - 1])
        for p in range(off, off + n):
            v = xs[x, p].astype(F32)
            for d in range(1, NX):
                v = v + xr[d - 1, p].astype(F32)
            zs[:, p] = v.astype(BF16).reshape(NZ, zrows, band)
        for d in range(1, NZ):
            t = lax.rem(z + d, NZ)
            send(
                zs.at[t, pl.ds(off, n)], zr.at[d - 1, pl.ds(off, n)],
                z_s.at[g, d - 1], z_r.at[g, d - 1], zdev(d),
            )

    def sum_over_z(g):
        off, n = GROUPS[g]
        for d in range(1, NZ):
            arrived(zr.at[d - 1, pl.ds(off, n)], z_s.at[g, d - 1], z_r.at[g, d - 1])
        for p in range(off, off + n):
            v = zs[z, p].astype(F32)
            for d in range(1, NZ):
                v = v + zr[d - 1, p].astype(F32)
            v = v * (1.0 / total_rows)
            if p == 0:
                v = v - unit(zrows, band, x * xrows + z * zrows, c * band)
            d32[p] = v
            w = v.astype(BF16)
            db[p] = w
            da[p, z, x] = w

    def unit(rows, cols, row0, col0):
        i = lax.broadcasted_iota(jnp.int32, (rows, cols), 0) + row0
        j = lax.broadcasted_iota(jnp.int32, (rows, cols), 1) + col0
        return (i == j).astype(F32)

    for j in range(2):
        if j == 1:
            arrived(xa.at[0, c, 1 - zl], sw_s, sw_r)
        to_minus(0, j)
        to_plus(0, j)
        to_sibling(0, j)
    def ring_step(h, j):
        if h < 4 or j == 0:
            arrived(xa.at[h, c, subs[j]], ring_s.at[0, h - 1, j], ring_r.at[0, h - 1, j])
            if h < 3 or (h == 3 and j == 0):
                to_minus(h, j)
            to_sibling(h, j)
        if h < 4 or j == 1:
            arrived(xa.at[NY - h, c, subs[j]], ring_s.at[1, h - 1, j], ring_r.at[1, h - 1, j])
            if h < 3 or (h == 3 and j == 1):
                to_plus(h, j)
            to_sibling(NY - h, j)

    def use(h, j):
        if (h, j) == (1, 0):
            from_sibling(0, 0)
            from_sibling(0, 1)
        from_sibling(h, j)
        if h < 4:
            from_sibling(NY - h, j)
        partial_margin(h - 1, j)

    def gather_x(g):
        off, n = GROUPS[g]
        v = da.at[pl.ds(off, n), z, x]
        for d in range(1, NX):
            send(v, v, gx_s.at[g, d - 1], gx_r.at[g, d - 1], xdev(d))

    def slab(g, i, h):
        off, n = GROUPS[g]
        t = lax.rem(z + (h if i == 0 else NZ - h), NZ)
        return t, pl.ds(off, n)

    def hop_send(g, i, h):
        t, ps = slab(g, i, h - 1)
        v = da.at[ps, t] if h < 4 else da.at[ps, t, pl.ds(2 * i, 2)]
        send(v, v, gz_s.at[g, i, h - 1], gz_r.at[g, i, h - 1], zdev(-1 if i == 0 else 1))

    def gather_z(g):
        off, n = GROUPS[g]
        for d in range(1, NX):
            t = lax.rem(x + NX - d, NX)
            arrived(da.at[pl.ds(off, n), z, t], gx_s.at[g, d - 1], gx_r.at[g, d - 1])
        for i in range(2):
            hop_send(g, i, 1)

    def hop(g, h):
        for i in range(2):
            t, ps = slab(g, i, h)
            v = da.at[ps, t] if h < 4 else da.at[ps, t, pl.ds(2 * i, 2)]
            arrived(v, gz_s.at[g, i, h - 1], gz_r.at[g, i, h - 1])
            if h < 4:
                hop_send(g, i, h + 1)

    def near_z(g):
        off, n = GROUPS[g]
        v = da.at[pl.ds(off, n), z, x]
        for d in range(1, NZ):
            send(v, v, hz_s.at[g - 1, d - 1], hz_r.at[g - 1, d - 1], zdev(d))

    def near_x(g):
        off, n = GROUPS[g]
        for d in range(1, NZ):
            t = lax.rem(z + NZ - d, NZ)
            arrived(da.at[pl.ds(off, n), t, x], hz_s.at[g - 1, d - 1], hz_r.at[g - 1, d - 1])
        v = da.at[pl.ds(off, n), :, x]
        for d in range(1, NX):
            send(v, v, hx_s.at[g - 1, d - 1], hx_r.at[g - 1, d - 1], xdev(d))

    def near_done(g):
        off, n = GROUPS[g]
        for d in range(1, NX):
            t = lax.rem(x + NX - d, NX)
            arrived(da.at[pl.ds(off, n), :, t], hx_s.at[g - 1, d - 1], hx_r.at[g - 1, d - 1])

    PARTS = ((0, 5), (5, 3))

    def rows_part(i):
        off, n = PARTS[i]
        return pl.ds(off, n)

    def left_send(i):
        ps = rows_part(i)
        for k in range(1, NY):
            send(db.at[ps], dj.at[k, c, ps], y_s.at[i, k - 1], y_r.at[i, k - 1], ydev(-k))
        off, n = PARTS[i]
        for p in range(off, off + n):
            dj[0, c, p] = db[p]
        if i == 1:
            send(db, dj.at[0, c], yf_s.at[0], yf_r.at[0], sibling)

    def left_pass():
        for k in range(1, NY):
            for i in range(2):
                arrived(dj.at[k, c, rows_part(i)], y_s.at[i, k - 1], y_r.at[i, k - 1])
            send(dj.at[k, c], dj.at[k, c], yf_s.at[k], yf_r.at[k], sibling)

    for h in range(1, 4):
        for j in range(2):
            ring_step(h, j)
            if (h, j) == (3, 0):
                sum_over_z(0)
                gather_x(0)
            use(h, j)
            if (h, j) == (2, 0):
                sum_over_x(0)
            if (h, j) == (3, 0):
                sum_over_x(1)
                gather_z(0)
    hop(0, 1)
    ring_step(4, 0)
    ring_step(4, 1)
    sum_over_z(1)
    near_z(1)
    hop(0, 2)
    use(4, 0)
    use(4, 1)
    sum_over_x(2)
    left_send(0)
    hop(0, 3)
    near_x(1)
    sum_over_x(3)
    sum_over_z(2)
    near_z(2)
    sum_over_z(3)
    near_z(3)
    left_send(1)
    near_x(2)
    near_x(3)
    hop(0, 4)
    left_pass()
    near_done(1)
    near_done(2)
    near_done(3)
    for k in range(NY):
        arrived(dj.at[k, 1 - c], yf_s.at[k], yf_r.at[k])

    def piece(b, t, u):
        return ca.at[t, u, pl.ds(4 * b, 4)]

    def zpiece(b, u, i, h, far):
        t = lax.rem(z + (h if i == 0 else NZ - h), NZ)
        return ca.at[t, u, pl.ds(4 * b + 2 * i, 2)] if far else piece(b, t, u)

    def a_send(d, i, h):
        v = zpiece(0, lax.rem(x + NX - d, NX), i, h - 1, h == 4)
        send(v, v, az_s.at[d, i, h - 1], az_r.at[d, i, h - 1], zdev(-1 if i == 0 else 1))

    def a_hop(d, h):
        for i in range(2):
            v = zpiece(0, lax.rem(x + NX - d, NX), i, h, h == 4)
            arrived(v, az_s.at[d, i, h - 1], az_r.at[d, i, h - 1])
            if h < 4:
                a_send(d, i, h + 1)

    def b_send(i, h):
        v = zpiece(1, x, i, h - 1, h == 4)
        send(v, v, bz_s.at[i, h - 1], bz_r.at[i, h - 1], zdev(-1 if i == 0 else 1))

    def b_along_x(r):
        v = piece(1, lax.rem(z + r, NZ), x)
        for d in (1, 3, 2):
            send(v, v, bx_s.at[r, d - 1], bx_r.at[r, d - 1], xdev(d))

    def b_hop(h):
        for i in range(2):
            arrived(zpiece(1, x, i, h, h == 4), bz_s.at[i, h - 1], bz_r.at[i, h - 1])
            if h < 4:
                b_send(i, h + 1)
        if h < 4:
            b_along_x(h)
            b_along_x(NZ - h)
        else:
            b_along_x(4)

    def plane_gather(between, a_done):
        for d in (1, 3, 2):
            send(piece(0, z, x), piece(0, z, x), ax_s.at[d - 1], ax_r.at[d - 1], xdev(d))
        for i in range(2):
            b_send(i, 1)
        for i in range(2):
            a_send(0, i, 1)
        b_along_x(0)
        b_hop(1)
        for d in (1, 3, 2):
            u = lax.rem(x + NX - d, NX)
            arrived(piece(0, z, u), ax_s.at[d - 1], ax_r.at[d - 1])
            for i in range(2):
                a_send(d, i, 1)
        a_hop(0, 1)
        between()
        for h in range(2, 6):
            if h < 5:
                b_hop(h)
                a_hop(0, h)
            for d in (1, 3, 2):
                a_hop(d, h - 1)
        a_done()
        for r in (0, 1, 7, 2, 6, 3, 5, 4):
            for d in (1, 3, 2):
                arrived(piece(1, lax.rem(z + r, NZ), lax.rem(x + NX - d, NX)), bx_s.at[r, d - 1], bx_r.at[r, d - 1])

    def rows_of(p, s):
        return jnp.concatenate([ca[:, 2 * s + i, p].reshape(xrows, band) for i in range(2)], axis=0)

    def dev_rows(p, s):
        return jnp.concatenate([da[p, :, 2 * s + i].reshape(xrows, band) for i in range(2)], axis=0)

    acc_sq = [None] * NY
    for k in range(NY):
        left = [dj[k, s].reshape(NY * zrows, band) for s in range(2)]
        part = dot(left[0], dev_rows(POS[k], 0)) + dot(left[1], dev_rows(POS[k], 1))
        for p in range(NY):
            m = POS[(k + SLOT[p]) % NY]
            rows = part[p * zrows : (p + 1) * zrows]
            acc_sq[m] = rows if acc_sq[m] is None else acc_sq[m] + rows
    for p in range(NY):
        v = 0.375 * acc_sq[p] - 0.5 * d32[p]
        if p == 0:
            v = v + unit(zrows, band, x * xrows + z * zrows, c * band)
        ca[z, x, p] = v.astype(BF16)

    kg = lax.rem(x * 2 + zh // 2 - y + NY, NY)
    pg = jnp.where(kg == 0, 0, jnp.where(kg <= 4, 2 * kg - 1, 2 * (NY - kg)))

    def mirror(core):
        q = lax.rem(zh, 2) * 2 + core
        return da[pg, :, q].reshape(xrows, band).astype(F32)

    def margin_work():
        ms[...] = mirror(1 - c).astype(BF16)
        send(ms, mr, m_s, m_r, sibling)

    def product(part):
        for cc in range(2):
            for p in range(4 * part, 4 * part + 4):
                k = SLOT[p]
                for s in range(2):
                    v = dot(xa[k, cc, s], rows_of(p, s))
                    if part == 0 and p == 0 and s == 0:
                        acc[cc] = v
                    else:
                        acc[cc] += v
            if part == 1:
                osb[cc] = acc[cc].astype(BF16)
                mine = (zl == c) & (c == cc)
                to = copy(
                    osb.at[cc], o_out.at[pl.ds(zl * half, half), :], out_s.at[cc], out_r.at[zl], {"zl": c, "c": cc}
                )

                @pl.when(jnp.logical_not(mine))
                def _():
                    to.start()

                @pl.when(mine)
                def _():
                    o_out[pl.ds(pl.multiple_of(zl * half, half), half), :] = osb[cc]

    def first_half():
        arrived(mr, m_s, m_r)
        v = jnp.where(zl == c, mirror(c), mr[...].astype(F32))
        rows0 = (y * 2 + zl) * band
        cols0 = (x * 8 + zh * 2 + c) * xrows
        m_out[...] = v.T + unit(band, xrows, rows0, cols0)
        product(0)

    plane_gather(margin_work, first_half)
    product(1)

    other = o_out.at[pl.ds((1 - zl) * half, half), :]
    arrived(other, out_s.at[0], out_r.at[1 - zl])

    @pl.when(zl != c)
    def _():
        arrived(o_out.at[pl.ds(zl * half, half), :], out_s.at[0], out_r.at[zl])

    for cc in range(2):

        @pl.when(jnp.logical_not((zl == c) & (c == cc)))
        def _():
            copy(
                osb.at[cc], o_out.at[pl.ds(zl * half, half), :], out_s.at[cc], out_r.at[zl], {"zl": c, "c": cc}
            ).wait_send()

    for g in range(len(GROUPS)):
        partial_sent(g)
    for h in sends:
        h.wait_send()


def shards(total_rows, orbitals):
    rows, band = orbitals.shape
    half = rows // 2
    xrows = 2 * band // NX
    zrows = xrows // NZ
    dma = pltpu.SemaphoreType.DMA
    v = pltpu.VMEM
    scratch = [
        v((NY, 2, 2, half, band), BF16),
        v((half, band), BF16),
        v((NX, NY, xrows, band), BF16),
        v((NX - 1, NY, xrows, band), BF16),
        v((NZ, NY, zrows, band), BF16),
        v((NZ - 1, NY, zrows, band), BF16),
        v((NY, zrows, band), BF16),
        v((NY, zrows, band), F32),
        v((NY, 2, NY, zrows, band), BF16),
        v((NY, NZ, NX, zrows, band), BF16),
        v((NZ, NX, NY, zrows, band), BF16),
        v((xrows, band), BF16),
        v((xrows, band), BF16),
        v((2, half, band), F32),
        v((2, half, band), BF16),
        dma((2,)),
        dma, dma,
        dma((2, 4, 2)), dma((2, 4, 2)),
        dma((NY, 2)), dma((NY, 2)),
        dma((4, NX - 1)), dma((4, NX - 1)),
        dma((4, NZ - 1)), dma((4, NZ - 1)),
        dma((2, NY - 1)), dma((2, NY - 1)),
        dma((NY,)), dma((NY,)),
        dma((1, NX - 1)), dma((1, NX - 1)),
        dma((1, 2, 4)), dma((1, 2, 4)),
        dma((3, NZ - 1)), dma((3, NZ - 1)),
        dma((3, NX - 1)), dma((3, NX - 1)),
        dma((NX - 1,)), dma((NX - 1,)),
        dma((NX, 2, 4)), dma((NX, 2, 4)),
        dma((2, 4)), dma((2, 4)),
        dma((NZ, NX - 1)), dma((NZ, NX - 1)),
        dma, dma,
        dma((2,)), dma((2,)),
    ]

    def body(*refs):
        kernel(total_rows, *refs)

    return pl.pallas_call(
        body,
        out_shape=(
            jax.ShapeDtypeStruct((band, xrows), F32),
            jax.ShapeDtypeStruct((rows, band), BF16),
        ),
        in_specs=[pl.BlockSpec(memory_space=pl.ANY)],
        out_specs=(pl.BlockSpec(memory_space=pltpu.VMEM), pl.BlockSpec(memory_space=pltpu.VMEM)),
        scratch_shapes=scratch,
        compiler_params=pltpu.CompilerParams(
            collective_id=0, has_side_effects=True, vmem_limit_bytes=56 * 1024 * 1024
        ),
    )(orbitals)


def solution(mesh):
    finer = Mesh(mesh.devices.reshape(NY, 2, NX, NZ // 2, 2), AXES)
    coeffs = ("x", "zh", "c")
    bands = ("y", "zl")

    def run(orbitals):
        total = orbitals.shape[0]
        return jax.shard_map(
            lambda o: shards(total, o),
            mesh=finer,
            in_specs=(P(coeffs, bands),),
            out_specs=(P(bands, coeffs), P(coeffs, bands)),
            check_vma=False,
        )(orbitals)

    return run
```

```python
import jax
import jax.numpy as jnp
from jax import lax
from jax.experimental import pallas as pl
from jax.experimental.pallas import tpu as pltpu
from jax.sharding import Mesh
from jax.sharding import PartitionSpec as P

AXES = ("y", "zl", "x", "zh", "c")
NY, NX, NZ = 8, 4, 8
SLOT = (0, 1, 7, 2, 6, 4, 3, 5)
POS = tuple(SLOT.index(k) for k in range(NY))
GROUPS = ((0, 3), (3, 2), (6, 2), (5, 1))
FACTORS = ((0, 0), (1, 0), (7, 0), (2, 0), (6, 0), (2, 6), (3, 0), (5, 0))
FAR = 5
MESH_ID = pl.DeviceIdType.MESH
F32 = jnp.float32
BF16 = jnp.bfloat16


def dot(a, b, dims=(((1,), (0,)), ((), ()))):
    return lax.dot_general(a, b, dims, preferred_element_type=F32)


def kernel(
    total_rows, x_hbm, m_out, o_out, xa, ph, xs, xr, zs, zr, db, d32, dq, dj, da, ca,
    ms, mr, acc, osb, in_sem, sw_s, sw_r, ring_s, ring_r, sib_s, sib_r, x_s, x_r, z_s, z_r,
    q_s, q_r, y_s, y_r, yf_s, yf_r, gx_s, gx_r, gz_s, gz_r, hz_s, hz_r, hx_s, hx_r,
    ax_s, ax_r, az_s, az_r, bz_s, bz_r, bx_s, bx_r, m_s, m_r, out_s, out_r,
):
    y = lax.axis_index("y")
    zl = lax.axis_index("zl")
    x = lax.axis_index("x")
    zh = lax.axis_index("zh")
    c = lax.axis_index("c")
    z = zh * 2 + zl
    half = ph.shape[0]
    band = ph.shape[1]
    xrows = xs.shape[2]
    zrows = zs.shape[2]
    sends = []

    def zdev(d):
        t = lax.rem(z + d + NZ, NZ)
        return {"zh": t // 2, "zl": lax.rem(t, 2)}

    def ydev(d):
        return {"y": lax.rem(y + d + NY, NY)}

    def xdev(d):
        return {"x": lax.rem(x + d + NX, NX)}

    sibling = {"c": 1 - c}

    def copy(src, dst, ssem, rsem, dev):
        return pltpu.make_async_remote_copy(
            src_ref=src, dst_ref=dst, send_sem=ssem, recv_sem=rsem, device_id=dev, device_id_type=MESH_ID
        )

    def send(src, dst, ssem, rsem, dev):
        h = copy(src, dst, ssem, rsem, dev)
        h.start()
        sends.append(h)

    def arrived(dst, ssem, rsem):
        copy(dst, dst, ssem, rsem, sibling).wait_recv()

    own_in = pltpu.make_async_copy(x_hbm.at[pl.ds(zl * half, half), :], xa.at[0, c, zl], in_sem.at[0])
    oth_in = pltpu.make_async_copy(x_hbm.at[pl.ds((1 - zl) * half, half), :], ph, in_sem.at[1])
    own_in.start()
    oth_in.start()

    barrier = pltpu.get_barrier_semaphore()
    peers = [sibling, {"zl": 1 - zl, "c": 1 - c}]
    peers += [ydev(d) for d in range(1, NY)]
    peers += [xdev(d) for d in range(1, NX)]
    peers += [zdev(d) for d in range(1, NZ)]
    for dev in peers:
        pl.semaphore_signal(barrier, inc=1, device_id=dev, device_id_type=MESH_ID)
    pl.semaphore_wait(barrier, len(peers))

    oth_in.wait()
    own_in.wait()
    send(ph, xa.at[0, c, zl], sw_s, sw_r, {"zl": 1 - zl})

    subs = (zl, 1 - zl)

    def to_minus(k, j):
        t = xa.at[k, c, subs[j]]
        u = xa.at[k + 1, c, subs[j]]
        send(t, u, ring_s.at[0, k, j], ring_r.at[0, k, j], ydev(-1))

    def to_plus(k, j):
        t = xa.at[(NY - k) % NY, c, subs[j]]
        u = xa.at[NY - k - 1, c, subs[j]]
        send(t, u, ring_s.at[1, k, j], ring_r.at[1, k, j], ydev(1))

    def to_sibling(k, j):
        t = xa.at[k, c, subs[j]]
        send(t, t, sib_s.at[k, j], sib_r.at[k, j], sibling)

    def from_sibling(k, j):
        arrived(xa.at[k, 1 - c, subs[j]], sib_s.at[k, j], sib_r.at[k, j])

    def partial_margin(g, j):
        off, n = GROUPS[g]
        s = subs[j]
        for p in range(off, off + n):
            k, r = FACTORS[p]
            v = dot(xa[k, 0, s], xa[r, 0, c], (((0,), (0,)), ((), ())))
            v = v + dot(xa[k, 1, s], xa[r, 1, c], (((0,), (0,)), ((), ())))
            v = v.astype(BF16)
            xs[2 * s, p] = v[:xrows]
            xs[2 * s + 1, p] = v[xrows:]
        for i in range(2):
            to = 2 * s + i
            d = lax.rem(to - x + NX, NX)
            at = jnp.maximum(d - 1, 0)
            h = copy(xs.at[to, pl.ds(off, n)], xr.at[at, pl.ds(off, n)], x_s.at[g, at], x_r.at[g, at], {"x": to})

            @pl.when(d > 0)
            def _():
                h.start()

    def partial_sent(g):
        off, n = GROUPS[g]
        for d in range(1, NX):
            t = xr.at[d - 1, pl.ds(off, n)]
            copy(t, t, x_s.at[g, d - 1], x_r.at[g, d - 1], sibling).wait_send()

    def sum_over_x(g):
        off, n = GROUPS[g]
        for d in range(1, NX):
            arrived(xr.at[d - 1, pl.ds(off, n)], x_s.at[g, d - 1], x_r.at[g, d - 1])
        for p in range(off, off + n):
            v = xs[x, p].astype(F32)
            for d in range(1, NX):
                v = v + xr[d - 1, p].astype(F32)
            zs[:, p] = v.astype(BF16).reshape(NZ, zrows, band)
        for d in range(1, NZ):
            t = lax.rem(z + d, NZ)
            send(
                zs.at[t, pl.ds(off, n)], zr.at[d - 1, pl.ds(off, n)],
                z_s.at[g, d - 1], z_r.at[g, d - 1], zdev(d),
            )

    def sum_over_z(g):
        off, n = GROUPS[g]
        for d in range(1, NZ):
            arrived(zr.at[d - 1, pl.ds(off, n)], z_s.at[g, d - 1], z_r.at[g, d - 1])
        for p in range(off, off + n):
            v = zs[z, p].astype(F32)
            for d in range(1, NZ):
                v = v + zr[d - 1, p].astype(F32)
            v = v * (1.0 / total_rows)
            if p == 0:
                v = v - unit(zrows, band, x * xrows + z * zrows, c * band)
            w = v.astype(BF16)
            if p == FAR:
                dq[...] = w
                send(dq, db.at[p], q_s, q_r, ydev(-2))
            else:
                d32[p] = v
                db[p] = w
                da[p, z, x] = w

    def place_far():
        arrived(db.at[FAR], q_s, q_r)
        da[FAR, z, x] = db[FAR]

    def unit(rows, cols, row0, col0):
        i = lax.broadcasted_iota(jnp.int32, (rows, cols), 0) + row0
        j = lax.broadcasted_iota(jnp.int32, (rows, cols), 1) + col0
        return (i == j).astype(F32)

    for j in range(2):
        if j == 1:
            arrived(xa.at[0, c, 1 - zl], sw_s, sw_r)
        to_minus(0, j)
        to_plus(0, j)
        to_sibling(0, j)
    def ring_step(h, j):
        if h < 4 or j == 0:
            arrived(xa.at[h, c, subs[j]], ring_s.at[0, h - 1, j], ring_r.at[0, h - 1, j])
            if h < 3 or (h == 3 and j == 0):
                to_minus(h, j)
            to_sibling(h, j)
        if h < 4 or j == 1:
            arrived(xa.at[NY - h, c, subs[j]], ring_s.at[1, h - 1, j], ring_r.at[1, h - 1, j])
            if h < 3 or (h == 3 and j == 1):
                to_plus(h, j)
            to_sibling(NY - h, j)

    def gather_x(g):
        off, n = GROUPS[g]
        v = da.at[pl.ds(off, n), z, x]
        for d in range(1, NX):
            send(v, v, gx_s.at[g, d - 1], gx_r.at[g, d - 1], xdev(d))

    def slab(g, i, h):
        off, n = GROUPS[g]
        t = lax.rem(z + (h if i == 0 else NZ - h), NZ)
        return t, pl.ds(off, n)

    def hop_send(g, i, h):
        t, ps = slab(g, i, h - 1)
        v = da.at[ps, t] if h < 4 else da.at[ps, t, pl.ds(2 * i, 2)]
        send(v, v, gz_s.at[g, i, h - 1], gz_r.at[g, i, h - 1], zdev(-1 if i == 0 else 1))

    def gather_z(g):
        off, n = GROUPS[g]
        for d in range(1, NX):
            t = lax.rem(x + NX - d, NX)
            arrived(da.at[pl.ds(off, n), z, t], gx_s.at[g, d - 1], gx_r.at[g, d - 1])
        for i in range(2):
            hop_send(g, i, 1)

    def hop(g, h):
        for i in range(2):
            t, ps = slab(g, i, h)
            v = da.at[ps, t] if h < 4 else da.at[ps, t, pl.ds(2 * i, 2)]
            arrived(v, gz_s.at[g, i, h - 1], gz_r.at[g, i, h - 1])
            if h < 4:
                hop_send(g, i, h + 1)

    def near_z(g):
        off, n = GROUPS[g]
        v = da.at[pl.ds(off, n), z, x]
        for d in range(1, NZ):
            send(db.at[pl.ds(off, n)], v, hz_s.at[g - 1, d - 1], hz_r.at[g - 1, d - 1], zdev(d))

    def near_x(g):
        off, n = GROUPS[g]
        for d in range(1, NZ):
            t = lax.rem(z + NZ - d, NZ)
            arrived(da.at[pl.ds(off, n), t, x], hz_s.at[g - 1, d - 1], hz_r.at[g - 1, d - 1])
        v = da.at[pl.ds(off, n), :, x]
        for d in range(1, NX):
            send(v, v, hx_s.at[g - 1, d - 1], hx_r.at[g - 1, d - 1], xdev(d))

    def near_done(g):
        off, n = GROUPS[g]
        for d in range(1, NX):
            t = lax.rem(x + NX - d, NX)
            arrived(da.at[pl.ds(off, n), :, t], hx_s.at[g - 1, d - 1], hx_r.at[g - 1, d - 1])

    PARTS = ((0, 6), (6, 2))

    def rows_part(i):
        off, n = PARTS[i]
        return pl.ds(off, n)

    def left_send(i):
        ps = rows_part(i)
        for k in range(1, NY):
            send(db.at[ps], dj.at[k, c, ps], y_s.at[i, k - 1], y_r.at[i, k - 1], ydev(-k))
        off, n = PARTS[i]
        for p in range(off, off + n):
            dj[0, c, p] = db[p]
        if i == 1:
            send(db, dj.at[0, c], yf_s.at[0], yf_r.at[0], sibling)

    def left_pass():
        for k in range(1, NY):
            for i in range(2):
                arrived(dj.at[k, c, rows_part(i)], y_s.at[i, k - 1], y_r.at[i, k - 1])
            send(dj.at[k, c], dj.at[k, c], yf_s.at[k], yf_r.at[k], sibling)

    def pair_in(h, j):
        from_sibling(h, j)
        from_sibling(NY - h, j)

    ring_step(1, 0)
    from_sibling(0, 0)
    from_sibling(0, 1)
    pair_in(1, 0)
    partial_margin(0, 0)
    ring_step(1, 1)
    pair_in(1, 1)
    partial_margin(0, 1)
    ring_step(2, 0)
    pair_in(2, 0)
    partial_margin(1, 0)
    sum_over_x(0)
    ring_step(2, 1)
    pair_in(2, 1)
    partial_margin(3, 0)
    partial_margin(3, 1)
    partial_margin(1, 1)
    ring_step(3, 0)
    sum_over_z(0)
    gather_x(0)
    pair_in(3, 0)
    partial_margin(2, 0)
    sum_over_x(3)
    sum_over_x(1)
    gather_z(0)
    ring_step(3, 1)
    pair_in(3, 1)
    partial_margin(2, 1)
    sum_over_z(3)
    sum_over_z(1)
    near_z(1)
    hop(0, 1)
    sum_over_x(2)
    place_far()
    near_z(3)
    left_send(0)
    ring_step(4, 0)
    ring_step(4, 1)
    hop(0, 2)
    near_x(1)
    sum_over_z(2)
    near_z(2)
    left_send(1)
    near_x(3)
    hop(0, 3)
    near_x(2)
    hop(0, 4)
    left_pass()
    near_done(1)
    near_done(3)
    near_done(2)
    for k in range(NY):
        arrived(dj.at[k, 1 - c], yf_s.at[k], yf_r.at[k])

    def piece(b, t, u):
        return ca.at[t, u, pl.ds(4 * b, 4)]

    def zpiece(b, u, i, h, far):
        t = lax.rem(z + (h if i == 0 else NZ - h), NZ)
        return ca.at[t, u, pl.ds(4 * b + 2 * i, 2)] if far else piece(b, t, u)

    def a_send(d, i, h):
        v = zpiece(0, lax.rem(x + NX - d, NX), i, h - 1, h == 4)
        send(v, v, az_s.at[d, i, h - 1], az_r.at[d, i, h - 1], zdev(-1 if i == 0 else 1))

    def a_hop(d, h):
        for i in range(2):
            v = zpiece(0, lax.rem(x + NX - d, NX), i, h, h == 4)
            arrived(v, az_s.at[d, i, h - 1], az_r.at[d, i, h - 1])
            if h < 4:
                a_send(d, i, h + 1)

    def b_send(i, h):
        v = zpiece(1, x, i, h - 1, h == 4)
        send(v, v, bz_s.at[i, h - 1], bz_r.at[i, h - 1], zdev(-1 if i == 0 else 1))

    def b_along_x(r):
        v = piece(1, lax.rem(z + r, NZ), x)
        for d in (1, 3, 2):
            send(v, v, bx_s.at[r, d - 1], bx_r.at[r, d - 1], xdev(d))

    def b_hop(h):
        for i in range(2):
            arrived(zpiece(1, x, i, h, h == 4), bz_s.at[i, h - 1], bz_r.at[i, h - 1])
            if h < 4:
                b_send(i, h + 1)
        if h < 4:
            b_along_x(h)
            b_along_x(NZ - h)
        else:
            b_along_x(4)

    def plane_gather(between, b_done):
        for d in (1, 3, 2):
            send(piece(0, z, x), piece(0, z, x), ax_s.at[d - 1], ax_r.at[d - 1], xdev(d))
        for i in range(2):
            b_send(i, 1)
        for i in range(2):
            a_send(0, i, 1)
        b_along_x(0)
        b_hop(1)
        for d in (1, 3, 2):
            u = lax.rem(x + NX - d, NX)
            arrived(piece(0, z, u), ax_s.at[d - 1], ax_r.at[d - 1])
            for i in range(2):
                a_send(d, i, 1)
        a_hop(0, 1)
        between()
        for h in range(2, 6):
            if h < 5:
                b_hop(h)
                a_hop(0, h)
            else:
                for r in (0, 1, 7, 2, 6, 3, 5, 4):
                    for d in (1, 3, 2):
                        v = piece(1, lax.rem(z + r, NZ), lax.rem(x + NX - d, NX))
                        arrived(v, bx_s.at[r, d - 1], bx_r.at[r, d - 1])
                b_done()
            for d in (1, 3, 2):
                a_hop(d, h - 1)

    def rows_of(p, s):
        return jnp.concatenate([ca[:, 2 * s + i, p].reshape(xrows, band) for i in range(2)], axis=0)

    def dev_rows(p, s):
        return jnp.concatenate([da[p, :, 2 * s + i].reshape(xrows, band) for i in range(2)], axis=0)

    acc_sq = [None] * NY
    for k in range(NY):
        left = [dj[k, s].reshape(NY * zrows, band) for s in range(2)]
        part = dot(left[0], dev_rows(POS[k], 0)) + dot(left[1], dev_rows(POS[k], 1))
        for p in range(NY):
            m = POS[(k + SLOT[p]) % NY]
            rows = part[p * zrows : (p + 1) * zrows]
            acc_sq[m] = rows if acc_sq[m] is None else acc_sq[m] + rows
    for p in range(NY):
        v = 0.375 * acc_sq[p] - 0.5 * (db[p].astype(F32) if p == FAR else d32[p])
        if p == 0:
            v = v + unit(zrows, band, x * xrows + z * zrows, c * band)
        ca[z, x, p] = v.astype(BF16)

    kg = lax.rem(x * 2 + zh // 2 - y + NY, NY)
    near = jnp.where(kg == 0, 0, jnp.where(kg <= 2, 2 * kg - 1, 2 * (NY - kg)))
    pg = jnp.where(kg == 3, 6, jnp.where(kg == 4, FAR, jnp.where(kg == 5, 7, near)))

    def mirror(core):
        q = lax.rem(zh, 2) * 2 + core
        return da[pg, :, q].reshape(xrows, band).astype(F32)

    def margin_work():
        from_sibling(4, 0)
        from_sibling(4, 1)
        ms[...] = mirror(1 - c).astype(BF16)
        send(ms, mr, m_s, m_r, sibling)

    def product(part):
        for cc in range(2):
            for p in range(4 * part, 4 * part + 4):
                k = SLOT[p]
                for s in range(2):
                    v = dot(xa[k, cc, s], rows_of(p, s))
                    if part == 1 and p == 4 and s == 0:
                        acc[cc] = v
                    else:
                        acc[cc] += v
            if part == 0:
                osb[cc] = acc[cc].astype(BF16)
                mine = (zl == c) & (c == cc)
                to = copy(
                    osb.at[cc], o_out.at[pl.ds(zl * half, half), :], out_s.at[cc], out_r.at[zl], {"zl": c, "c": cc}
                )

                @pl.when(jnp.logical_not(mine))
                def _():
                    to.start()

                @pl.when(mine)
                def _():
                    o_out[pl.ds(pl.multiple_of(zl * half, half), half), :] = osb[cc]

    def first_half():
        arrived(mr, m_s, m_r)
        v = jnp.where(zl == c, mirror(c), mr[...].astype(F32))
        rows0 = (y * 2 + zl) * band
        cols0 = (x * 8 + zh * 2 + c) * xrows
        m_out[...] = v.T + unit(band, xrows, rows0, cols0)
        product(1)

    plane_gather(margin_work, first_half)
    product(0)

    other = o_out.at[pl.ds((1 - zl) * half, half), :]
    arrived(other, out_s.at[0], out_r.at[1 - zl])

    @pl.when(zl != c)
    def _():
        arrived(o_out.at[pl.ds(zl * half, half), :], out_s.at[0], out_r.at[zl])

    for cc in range(2):

        @pl.when(jnp.logical_not((zl == c) & (c == cc)))
        def _():
            copy(
                osb.at[cc], o_out.at[pl.ds(zl * half, half), :], out_s.at[cc], out_r.at[zl], {"zl": c, "c": cc}
            ).wait_send()

    for g in range(len(GROUPS)):
        partial_sent(g)
    for h in sends:
        h.wait_send()


def shards(total_rows, orbitals):
    rows, band = orbitals.shape
    half = rows // 2
    xrows = 2 * band // NX
    zrows = xrows // NZ
    dma = pltpu.SemaphoreType.DMA
    v = pltpu.VMEM
    scratch = [
        v((NY, 2, 2, half, band), BF16),
        v((half, band), BF16),
        v((NX, NY, xrows, band), BF16),
        v((NX - 1, NY, xrows, band), BF16),
        v((NZ, NY, zrows, band), BF16),
        v((NZ - 1, NY, zrows, band), BF16),
        v((NY, zrows, band), BF16),
        v((NY, zrows, band), F32),
        v((zrows, band), BF16),
        v((NY, 2, NY, zrows, band), BF16),
        v((NY, NZ, NX, zrows, band), BF16),
        v((NZ, NX, NY, zrows, band), BF16),
        v((xrows, band), BF16),
        v((xrows, band), BF16),
        v((2, half, band), F32),
        v((2, half, band), BF16),
        dma((2,)),
        dma, dma,
        dma((2, 4, 2)), dma((2, 4, 2)),
        dma((NY, 2)), dma((NY, 2)),
        dma((4, NX - 1)), dma((4, NX - 1)),
        dma((4, NZ - 1)), dma((4, NZ - 1)),
        dma, dma,
        dma((2, NY - 1)), dma((2, NY - 1)),
        dma((NY,)), dma((NY,)),
        dma((1, NX - 1)), dma((1, NX - 1)),
        dma((1, 2, 4)), dma((1, 2, 4)),
        dma((3, NZ - 1)), dma((3, NZ - 1)),
        dma((3, NX - 1)), dma((3, NX - 1)),
        dma((NX - 1,)), dma((NX - 1,)),
        dma((NX, 2, 4)), dma((NX, 2, 4)),
        dma((2, 4)), dma((2, 4)),
        dma((NZ, NX - 1)), dma((NZ, NX - 1)),
        dma, dma,
        dma((2,)), dma((2,)),
    ]

    def body(*refs):
        kernel(total_rows, *refs)

    margin, corrected = pl.pallas_call(
        body,
        out_shape=(v((band, xrows), F32), v((rows, band), BF16)),
        in_specs=[pl.BlockSpec(memory_space=pl.ANY)],
        out_specs=(pl.BlockSpec(memory_space=pltpu.VMEM), pl.BlockSpec(memory_space=pltpu.VMEM)),
        scratch_shapes=scratch,
        compiler_params=pltpu.CompilerParams(
            collective_id=0, has_side_effects=True, vmem_limit_bytes=56 * 1024 * 1024
        ),
    )(orbitals)
    return pl.pallas_call(
        write_out,
        out_shape=(
            jax.ShapeDtypeStruct((band, xrows), F32),
            jax.ShapeDtypeStruct((rows, band), BF16),
        ),
        in_specs=[pl.BlockSpec(memory_space=pltpu.VMEM)] * 2,
        out_specs=(pl.BlockSpec(memory_space=pl.ANY),) * 2,
        scratch_shapes=[dma((2,))],
        compiler_params=pltpu.CompilerParams(vmem_limit_bytes=4 * 1024 * 1024),
    )(margin, corrected)


def write_out(m_ref, o_ref, m_out, o_out, sem):
    copies = [
        pltpu.make_async_copy(m_ref, m_out, sem.at[0]),
        pltpu.make_async_copy(o_ref, o_out, sem.at[1]),
    ]
    for h in copies:
        h.start()
    for h in copies:
        h.wait()


def solution(mesh):
    finer = Mesh(mesh.devices.reshape(NY, 2, NX, NZ // 2, 2), AXES)
    coeffs = ("x", "zh", "c")
    bands = ("y", "zl")

    def run(orbitals):
        total = orbitals.shape[0]
        return jax.shard_map(
            lambda o: shards(total, o),
            mesh=finer,
            in_specs=(P(coeffs, bands),),
            out_specs=(P(bands, coeffs), P(coeffs, bands)),
            check_vma=False,
        )(orbitals)

    return run
```

```python
import jax
import jax.numpy as jnp
from jax import lax
from jax.experimental import pallas as pl
from jax.experimental.pallas import tpu as pltpu
from jax.sharding import Mesh
from jax.sharding import PartitionSpec as P

AXES = ("y", "zl", "x", "zh", "c")
NY, NX, NZ = 8, 4, 8
SLOT = (0, 1, 7, 2, 6, 4, 3, 5)
POS = tuple(SLOT.index(k) for k in range(NY))
GROUPS = ((0, 1), (3, 2), (6, 2), (5, 1), (1, 2))
FACTORS = ((0, 0), (1, 0), (7, 0), (2, 0), (6, 0), (2, 6), (3, 0), (5, 0))
FAR = 5
MESH_ID = pl.DeviceIdType.MESH
F32 = jnp.float32
BF16 = jnp.bfloat16


def dot(a, b, dims=(((1,), (0,)), ((), ()))):
    return lax.dot_general(a, b, dims, preferred_element_type=F32)


def kernel(
    total_rows, x_hbm, m_out, o_out, xa, ph, xs, xr, zs, zr, db, d32, dq, dj, da, ca,
    ms, mr, acc, osb, rb, land, in_sem, sw_s, sw_r, ring_s, ring_r, sib_s, sib_r, x_s, x_r, z_s, z_r,
    q_s, q_r, y_s, y_r, yf_s, yf_r, gx_s, gx_r, gz_s, gz_r, hz_s, hz_r, hp_s, hp_r,
    ax_s, ax_r, az_s, az_r, bz_s, bz_r, bx_s, bx_r, m_s, m_r, os_s, os_r, oz_s, oz_r,
):
    y = lax.axis_index("y")
    zl = lax.axis_index("zl")
    x = lax.axis_index("x")
    zh = lax.axis_index("zh")
    c = lax.axis_index("c")
    z = zh * 2 + zl
    half = ph.shape[0]
    band = ph.shape[1]
    xrows = xs.shape[2]
    zrows = zs.shape[2]

    def zdev(d):
        t = lax.rem(z + d + NZ, NZ)
        return {"zh": t // 2, "zl": lax.rem(t, 2)}

    def ydev(d):
        return {"y": lax.rem(y + d + NY, NY)}

    def xdev(d):
        return {"x": lax.rem(x + d + NX, NX)}

    sibling = {"c": 1 - c}

    def copy(src, dst, ssem, rsem, dev):
        return pltpu.make_async_remote_copy(
            src_ref=src, dst_ref=dst, send_sem=ssem, recv_sem=rsem, device_id=dev, device_id_type=MESH_ID
        )

    def send(src, dst, ssem, rsem, dev):
        copy(src, dst, ssem, rsem, dev).start()

    def arrived(dst, ssem, rsem):
        copy(dst, dst, ssem, rsem, sibling).wait_recv()

    own_in = pltpu.make_async_copy(x_hbm.at[pl.ds(zl * half, half), :], xa.at[0, c, zl], in_sem.at[0])
    oth_in = pltpu.make_async_copy(x_hbm.at[pl.ds((1 - zl) * half, half), :], ph, in_sem.at[1])
    own_in.start()
    oth_in.start()

    barrier = pltpu.get_barrier_semaphore()
    peers = [sibling]
    peers += [ydev(d) for d in range(1, NY)]
    peers += [xdev(d) for d in range(1, NX)]
    peers += [zdev(d) for d in range(1, NZ)]
    for dev in peers:
        pl.semaphore_signal(barrier, inc=1, device_id=dev, device_id_type=MESH_ID)
    pl.semaphore_wait(barrier, len(peers))

    oth_in.wait()
    own_in.wait()
    send(ph, xa.at[0, c, zl], sw_s, sw_r, {"zl": 1 - zl})

    subs = (zl, 1 - zl)

    def to_minus(k, j):
        t = xa.at[k, c, subs[j]]
        u = xa.at[k + 1, c, subs[j]]
        send(t, u, ring_s, ring_r.at[0, k, j], ydev(-1))

    def to_plus(k, j):
        t = xa.at[(NY - k) % NY, c, subs[j]]
        u = xa.at[NY - k - 1, c, subs[j]]
        send(t, u, ring_s, ring_r.at[1, k, j], ydev(1))

    def to_sibling(k, j):
        t = xa.at[k, c, subs[j]]
        send(t, t, sib_s, sib_r.at[k, j], sibling)

    def from_sibling(k, j):
        arrived(xa.at[k, 1 - c, subs[j]], sib_s, sib_r.at[k, j])

    def partial_margin(g, j):
        off, n = GROUPS[g]
        s = subs[j]
        for p in range(off, off + n):
            k, r = FACTORS[p]
            v = dot(xa[k, 0, s], xa[r, 0, c], (((0,), (0,)), ((), ())))
            v = v + dot(xa[k, 1, s], xa[r, 1, c], (((0,), (0,)), ((), ())))
            v = v.astype(BF16)
            xs[2 * s, p] = v[:xrows]
            xs[2 * s + 1, p] = v[xrows:]
        for i in range(2):
            to = 2 * s + i
            d = lax.rem(to - x + NX, NX)
            at = jnp.maximum(d - 1, 0)
            h = copy(xs.at[to, pl.ds(off, n)], xr.at[at, pl.ds(off, n)], x_s, x_r.at[g], {"x": to})

            @pl.when(d > 0)
            def _():
                h.start()

    def sum_over_x(g):
        off, n = GROUPS[g]
        arrived(xr.at[:, pl.ds(off, n)], x_s, x_r.at[g])
        for p in range(off, off + n):
            v = xs[x, p].astype(F32)
            for d in range(1, NX):
                v = v + xr[d - 1, p].astype(F32)
            zs[:, p] = v.astype(BF16).reshape(NZ, zrows, band)
        for d in range(1, NZ):
            t = lax.rem(z + d, NZ)
            send(
                zs.at[t, pl.ds(off, n)], zr.at[d - 1, pl.ds(off, n)],
                z_s, z_r.at[g], zdev(d),
            )

    def sum_over_z(g):
        off, n = GROUPS[g]
        arrived(zr.at[:, pl.ds(off, n)], z_s, z_r.at[g])
        for p in range(off, off + n):
            v = zs[z, p].astype(F32)
            for d in range(1, NZ):
                v = v + zr[d - 1, p].astype(F32)
            v = v * (1.0 / total_rows)
            if p == 0:
                v = v - unit(zrows, band, x * xrows + z * zrows, c * band)
            w = v.astype(BF16)
            if p == FAR:
                dq[...] = w
                send(dq, db.at[p], q_s, q_r, ydev(-2))
            else:
                d32[p] = v
                db[p] = w
                da[p, z, x] = w

    def place_far():
        arrived(db.at[FAR], q_s, q_r)
        da[FAR, z, x] = db[FAR]

    def unit(rows, cols, row0, col0):
        i = lax.broadcasted_iota(jnp.int32, (rows, cols), 0) + row0
        j = lax.broadcasted_iota(jnp.int32, (rows, cols), 1) + col0
        return (i == j).astype(F32)

    for j in range(2):
        if j == 1:
            arrived(xa.at[0, c, 1 - zl], sw_s, sw_r)
        to_minus(0, j)
        to_plus(0, j)
        to_sibling(0, j)
    def ring_step(h, j):
        if h < 4 or j == 0:
            arrived(xa.at[h, c, subs[j]], ring_s, ring_r.at[0, h - 1, j])
            if h < 3 or (h == 3 and j == 0):
                to_minus(h, j)
            to_sibling(h, j)
        if h < 4 or j == 1:
            arrived(xa.at[NY - h, c, subs[j]], ring_s, ring_r.at[1, h - 1, j])
            if h < 3 or (h == 3 and j == 1):
                to_plus(h, j)
            to_sibling(NY - h, j)

    def gather_x(g):
        off, n = GROUPS[g]
        v = da.at[pl.ds(off, n), z, x]
        for d in range(1, NX):
            send(v, v, gx_s, gx_r.at[g // 4], xdev(d))

    def slab(g, i, h):
        off, n = GROUPS[g]
        t = lax.rem(z + (h if i == 0 else NZ - h), NZ)
        return t, pl.ds(off, n)

    def hop_send(g, i, h):
        t, ps = slab(g, i, h - 1)
        v = da.at[ps, t] if h < 4 else da.at[ps, t, pl.ds(2 * i, 2)]
        send(v, v, gz_s, gz_r.at[g // 4, i, h - 1], zdev(-1 if i == 0 else 1))

    def gather_z(g):
        off, n = GROUPS[g]
        arrived(da.at[pl.ds(off, n), z, pl.ds(0, NX - 1)], gx_s, gx_r.at[g // 4])
        for i in range(2):
            hop_send(g, i, 1)

    def hop(g, h):
        for i in range(2):
            t, ps = slab(g, i, h)
            v = da.at[ps, t] if h < 4 else da.at[ps, t, pl.ds(2 * i, 2)]
            arrived(v, gz_s, gz_r.at[g // 4, i, h - 1])
            if h < 4:
                hop_send(g, i, h + 1)

    def near_z(g):
        off, n = GROUPS[g]
        v = da.at[pl.ds(off, n), z, x]
        for d in range(1, NZ):
            send(db.at[pl.ds(off, n)], v, hz_s, hz_r.at[g - 1, d - 1], zdev(d))

    def pieces_x(g, rs):
        off, n = GROUPS[g]
        for r in rs:
            t = lax.rem(z + r, NZ)
            v = da.at[pl.ds(off, n), t, x]
            if r:
                arrived(v, hz_s, hz_r.at[g - 1, NZ - 1 - r])
            for d in (1, 3, 2):
                send(v if r else db.at[pl.ds(off, n)], v, hp_s, hp_r.at[g - 1], xdev(d))

    def pieces_done(g):
        off, n = GROUPS[g]
        arrived(da.at[pl.ds(off, n), :, pl.ds(0, NX - 1)], hp_s, hp_r.at[g - 1])

    PARTS = ((0, 6), (6, 2))

    def rows_part(i):
        off, n = PARTS[i]
        return pl.ds(off, n)

    def left_send(i):
        ps = rows_part(i)
        for k in range(1, NY):
            send(db.at[ps], dj.at[k, c, ps], y_s, y_r, ydev(-k))
        off, n = PARTS[i]
        for p in range(off, off + n):
            dj[0, c, p] = db[p]
        if i == 1:
            send(db, dj.at[0, c], yf_s, yf_r.at[0], sibling)

    def left_pass():
        v = dj.at[pl.ds(1, NY - 1), c]
        arrived(v, y_s, y_r)
        send(v, v, yf_s, yf_r.at[1], sibling)

    def pair_in(h, j):
        from_sibling(h, j)
        from_sibling(NY - h, j)

    ring_step(1, 0)
    from_sibling(0, 0)
    from_sibling(0, 1)
    partial_margin(0, 0)
    partial_margin(0, 1)
    pair_in(1, 0)
    partial_margin(4, 0)
    ring_step(1, 1)
    pair_in(1, 1)
    partial_margin(4, 1)
    sum_over_x(0)
    ring_step(2, 0)
    pair_in(2, 0)
    partial_margin(1, 0)
    sum_over_z(0)
    gather_x(0)
    ring_step(2, 1)
    sum_over_x(4)
    pair_in(2, 1)
    partial_margin(3, 0)
    partial_margin(3, 1)
    partial_margin(1, 1)
    gather_z(0)
    ring_step(3, 0)
    hop(0, 1)
    sum_over_z(4)
    gather_x(4)
    pair_in(3, 0)
    partial_margin(2, 0)
    sum_over_x(3)
    sum_over_x(1)
    hop(0, 2)
    ring_step(3, 1)
    gather_z(4)
    pair_in(3, 1)
    partial_margin(2, 1)
    sum_over_z(3)
    sum_over_z(1)
    near_z(1)
    pieces_x(1, (0,))
    hop(0, 3)
    hop(4, 1)
    sum_over_x(2)
    place_far()
    near_z(3)
    pieces_x(3, (0,))
    left_send(0)
    ring_step(4, 0)
    ring_step(4, 1)
    hop(0, 4)
    pieces_x(1, (1, 7, 2, 6))
    hop(4, 2)
    pieces_x(1, (3, 5, 4))
    pieces_x(3, (1, 7))
    sum_over_z(2)
    near_z(2)
    pieces_x(2, (0,))
    left_send(1)
    hop(4, 3)
    pieces_x(3, (2, 6, 3, 5, 4))
    pieces_x(2, (1, 7, 2, 6))
    hop(4, 4)
    pieces_x(2, (3, 5, 4))
    left_pass()
    pieces_done(1)
    pieces_done(3)
    pieces_done(2)
    arrived(dj.at[0, 1 - c], yf_s, yf_r.at[0])
    arrived(dj.at[pl.ds(1, NY - 1), 1 - c], yf_s, yf_r.at[1])

    def piece(b, t, u):
        return ca.at[t, u, pl.ds(4 * b, 4)]

    def zpiece(b, u, i, h, far):
        t = lax.rem(z + (h if i == 0 else NZ - h), NZ)
        return ca.at[t, u, pl.ds(4 * b + 2 * i, 2)] if far else piece(b, t, u)

    def a_send(d, i, h):
        v = zpiece(0, lax.rem(x + NX - d, NX), i, h - 1, h == 4)
        send(v, v, az_s, az_r.at[d, i, h - 1], zdev(-1 if i == 0 else 1))

    def a_hop(d, h):
        for i in range(2):
            v = zpiece(0, lax.rem(x + NX - d, NX), i, h, h == 4)
            arrived(v, az_s, az_r.at[d, i, h - 1])
            if h < 4:
                a_send(d, i, h + 1)

    def b_send(i, h):
        v = zpiece(1, x, i, h - 1, h == 4)
        send(v, v, bz_s, bz_r.at[i, h - 1], zdev(-1 if i == 0 else 1))

    def b_along_x(r):
        v = piece(1, lax.rem(z + r, NZ), x)
        for d in (1, 3, 2):
            send(v, v, bx_s, bx_r, xdev(d))

    def b_hop(h):
        for i in range(2):
            arrived(zpiece(1, x, i, h, h == 4), bz_s, bz_r.at[i, h - 1])
            if h < 4:
                b_send(i, h + 1)
        if h < 4:
            b_along_x(h)
            b_along_x(NZ - h)
        else:
            b_along_x(4)

    def plane_gather(between, b_done):
        for d in (1, 3, 2):
            send(piece(0, z, x), piece(0, z, x), ax_s, ax_r.at[d - 1], xdev(d))
        for i in range(2):
            b_send(i, 1)
        for i in range(2):
            a_send(0, i, 1)
        b_along_x(0)
        b_hop(1)
        for d in (1, 3, 2):
            u = lax.rem(x + NX - d, NX)
            arrived(piece(0, z, u), ax_s, ax_r.at[d - 1])
            for i in range(2):
                a_send(d, i, 1)
        a_hop(0, 1)
        between()
        for h in range(2, 6):
            if h < 5:
                b_hop(h)
                a_hop(0, h)
            else:
                arrived(ca.at[:, pl.ds(0, NX - 1), pl.ds(4, 4)], bx_s, bx_r)
                b_done()
            for d in (1, 3, 2):
                a_hop(d, h - 1)

    def rows_of(p, s):
        return jnp.concatenate([ca[:, 2 * s + i, p].reshape(xrows, band) for i in range(2)], axis=0)

    def dev_rows(p, s):
        return jnp.concatenate([da[p, :, 2 * s + i].reshape(xrows, band) for i in range(2)], axis=0)

    acc_sq = [None] * NY
    for k in range(NY):
        left = [dj[k, s].reshape(NY * zrows, band) for s in range(2)]
        part = dot(left[0], dev_rows(POS[k], 0)) + dot(left[1], dev_rows(POS[k], 1))
        for p in range(NY):
            m = POS[(k + SLOT[p]) % NY]
            rows = part[p * zrows : (p + 1) * zrows]
            acc_sq[m] = rows if acc_sq[m] is None else acc_sq[m] + rows
    for p in range(NY):
        v = 0.375 * acc_sq[p] - 0.5 * (db[p].astype(F32) if p == FAR else d32[p])
        if p == 0:
            v = v + unit(zrows, band, x * xrows + z * zrows, c * band)
        ca[z, x, p] = v.astype(BF16)

    kg = lax.rem(x * 2 + zh // 2 - y + NY, NY)
    near = jnp.where(kg == 0, 0, jnp.where(kg <= 2, 2 * kg - 1, 2 * (NY - kg)))
    pg = jnp.where(kg == 3, 6, jnp.where(kg == 4, FAR, jnp.where(kg == 5, 7, near)))

    def mirror(core):
        q = lax.rem(zh, 2) * 2 + core
        return da[pg, :, q].reshape(xrows, band).astype(F32)

    def margin_work():
        from_sibling(4, 0)
        from_sibling(4, 1)
        ms[...] = mirror(1 - c).astype(BF16)
        send(ms, mr, m_s, m_r, sibling)

    home = zl == c
    kept = pl.ds(pl.multiple_of(zl * half, half), half)
    swapped = pl.ds(pl.multiple_of((1 - zl) * half, half), half)
    to_pair = {"zl": 1 - zl}

    def product(part):
        for i, cc in enumerate((1 - c, c)):
            for p in range(4 * part, 4 * part + 4):
                k = SLOT[p]
                for s in range(2):
                    v = dot(xa[k, cc, s], rows_of(p, s))
                    if part == 1 and p == 4 and s == 0:
                        acc[i] = v
                    else:
                        acc[i] += v
            if part == 0:
                osb[i] = acc[i].astype(BF16)
                if i == 0:
                    copy(osb.at[0], rb, os_s, os_r, sibling).start()
                else:

                    @pl.when(home)
                    def _():
                        o_out[kept, :] = osb[1]

                    @pl.when(jnp.logical_not(home))
                    def _():
                        copy(osb.at[1], land, oz_s, oz_r, to_pair).start()

    def first_half():
        arrived(mr, m_s, m_r)
        v = jnp.where(zl == c, mirror(c), mr[...].astype(F32))
        rows0 = (y * 2 + zl) * band
        cols0 = (x * 8 + zh * 2 + c) * xrows
        m_out[...] = v.T + unit(band, xrows, rows0, cols0)
        product(1)

    plane_gather(margin_work, first_half)

    @pl.when(home)
    def _():
        arrived(rb, os_s, os_r)
        copy(rb, land, oz_s, oz_r, to_pair).start()

    product(0)

    low = pl.ds(0, NZ - 1)
    three = pl.ds(0, NX - 1)
    for v, sem in (
        (ph, sw_s),
        (xa.at[pl.ds(0, 7), :, 0], ring_s),
        (xa.at[:, :, 0], sib_s),
        (xr, x_s),
        (zr, z_s),
        (dq, q_s),
        (dj.at[pl.ds(1, NY - 1), 0], y_s),
        (dj.at[:, 0], yf_s),
        (da.at[three, 0, three], gx_s),
        (da.at[three, low], gz_s),
        (da.at[pl.ds(0, 5), low, 0], hz_s),
        (da.at[pl.ds(0, 5), :, three], hp_s),
        (ca.at[0, three, pl.ds(0, 4)], ax_s),
        (ca.at[low, :, pl.ds(0, 4)], az_s),
        (ca.at[low, 0, pl.ds(0, 4)], bz_s),
        (ca.at[:, three, pl.ds(0, 4)], bx_s),
        (ms, m_s),
    ):
        copy(v, v, sem, m_r, sibling).wait_send()

    @pl.when(jnp.logical_not(home))
    def _():
        arrived(rb, os_s, os_r)
        o_out[kept, :] = rb[...]

    arrived(land, oz_s, oz_r)
    o_out[swapped, :] = land[...]

    copy(rb, rb, os_s, os_r, sibling).wait_send()
    copy(rb, rb, oz_s, oz_r, sibling).wait_send()


def shards(total_rows, orbitals):
    rows, band = orbitals.shape
    half = rows // 2
    xrows = 2 * band // NX
    zrows = xrows // NZ
    dma = pltpu.SemaphoreType.DMA
    v = pltpu.VMEM
    scratch = [
        v((NY, 2, 2, half, band), BF16),
        v((half, band), BF16),
        v((NX, NY, xrows, band), BF16),
        v((NX - 1, NY, xrows, band), BF16),
        v((NZ, NY, zrows, band), BF16),
        v((NZ - 1, NY, zrows, band), BF16),
        v((NY, zrows, band), BF16),
        v((NY, zrows, band), F32),
        v((zrows, band), BF16),
        v((NY, 2, NY, zrows, band), BF16),
        v((NY, NZ, NX, zrows, band), BF16),
        v((NZ, NX, NY, zrows, band), BF16),
        v((xrows, band), BF16),
        v((xrows, band), BF16),
        v((2, half, band), F32),
        v((2, half, band), BF16),
        v((half, band), BF16),
        v((half, band), BF16),
        dma((2,)),
        dma, dma,
        dma, dma((2, 4, 2)),
        dma, dma((NY, 2)),
        dma, dma((5,)),
        dma, dma((5,)),
        dma, dma,
        dma, dma,
        dma, dma((2,)),
        dma, dma((2,)),
        dma, dma((2, 2, 4)),
        dma, dma((3, NZ - 1)),
        dma, dma((3,)),
        dma, dma((NX - 1,)),
        dma, dma((NX, 2, 4)),
        dma, dma((2, 4)),
        dma, dma,
        dma, dma,
        dma, dma,
        dma, dma,
    ]

    def body(*refs):
        kernel(total_rows, *refs)

    margin, corrected = pl.pallas_call(
        body,
        out_shape=(v((band, xrows), F32), v((rows, band), BF16)),
        in_specs=[pl.BlockSpec(memory_space=pl.ANY)],
        out_specs=(pl.BlockSpec(memory_space=pltpu.VMEM), pl.BlockSpec(memory_space=pltpu.VMEM)),
        scratch_shapes=scratch,
        compiler_params=pltpu.CompilerParams(
            collective_id=0, has_side_effects=True, vmem_limit_bytes=56 * 1024 * 1024
        ),
    )(orbitals)
    return pl.pallas_call(
        write_out,
        out_shape=(
            jax.ShapeDtypeStruct((band, xrows), F32),
            jax.ShapeDtypeStruct((rows, band), BF16),
        ),
        in_specs=[pl.BlockSpec(memory_space=pltpu.VMEM)] * 2,
        out_specs=(pl.BlockSpec(memory_space=pl.ANY),) * 2,
        scratch_shapes=[dma((2,))],
        compiler_params=pltpu.CompilerParams(vmem_limit_bytes=4 * 1024 * 1024),
    )(margin, corrected)


def write_out(m_ref, o_ref, m_out, o_out, sem):
    copies = [
        pltpu.make_async_copy(m_ref, m_out, sem.at[0]),
        pltpu.make_async_copy(o_ref, o_out, sem.at[1]),
    ]
    for h in copies:
        h.start()
    for h in copies:
        h.wait()


def solution(mesh):
    finer = Mesh(mesh.devices.reshape(NY, 2, NX, NZ // 2, 2), AXES)
    coeffs = ("x", "zh", "c")
    bands = ("y", "zl")

    def run(orbitals):
        total = orbitals.shape[0]
        return jax.shard_map(
            lambda o: shards(total, o),
            mesh=finer,
            in_specs=(P(coeffs, bands),),
            out_specs=(P(bands, coeffs), P(coeffs, bands)),
            check_vma=False,
        )(orbitals)

    return run
```

```python
import jax
import jax.numpy as jnp
from jax import lax
from jax.experimental import pallas as pl
from jax.experimental.pallas import tpu as pltpu
from jax.sharding import Mesh
from jax.sharding import PartitionSpec as P

AXES = ("y", "zl", "x", "zh", "c")
NY, NX, NZ = 8, 4, 8
SLOT = (0, 1, 7, 2, 6, 4, 3, 5)
POS = tuple(SLOT.index(k) for k in range(NY))
GROUPS = ((0, 1), (3, 2), (6, 2), (5, 1), (1, 2))
FACTORS = ((0, 0), (1, 0), (7, 0), (2, 0), (6, 0), (2, 6), (3, 0), (5, 0))
FAR = 5
HALVES = ((0, 3), (3, 5))
MESH_ID = pl.DeviceIdType.MESH
F32 = jnp.float32
BF16 = jnp.bfloat16


def dot(a, b, dims=(((1,), (0,)), ((), ()))):
    return lax.dot_general(a, b, dims, preferred_element_type=F32)


def kernel(
    total_rows, x_hbm, m_out, o_out, xa, ph, xs, xr, zs, zr, db, d32, dq, dj, da, ca,
    ms, mr, acc, osb, rb, land, in_sem, sw_s, sw_r, ring_s, ring_r, sib_s, sib_r, x_s, x_r, z_s, z_r,
    q_s, q_r, y_s, y_r, yf_s, yf_r, gx_s, gx_r, gz_s, gz_r, hz_s, hz_r, hp_s, hp_r,
    ax_s, ax_r, az_s, az_r, bz_s, bz_r, bx_s, bx_r, m_s, m_r, os_s, os_r, oz_s, oz_r,
):
    y = lax.axis_index("y")
    zl = lax.axis_index("zl")
    x = lax.axis_index("x")
    zh = lax.axis_index("zh")
    c = lax.axis_index("c")
    z = zh * 2 + zl
    half = ph.shape[0]
    band = ph.shape[1]
    xrows = xs.shape[2]
    zrows = zs.shape[2]

    def zdev(d):
        t = lax.rem(z + d + NZ, NZ)
        return {"zh": t // 2, "zl": lax.rem(t, 2)}

    def ydev(d):
        return {"y": lax.rem(y + d + NY, NY)}

    def xdev(d):
        return {"x": lax.rem(x + d + NX, NX)}

    sibling = {"c": 1 - c}

    def copy(src, dst, ssem, rsem, dev):
        return pltpu.make_async_remote_copy(
            src_ref=src, dst_ref=dst, send_sem=ssem, recv_sem=rsem, device_id=dev, device_id_type=MESH_ID
        )

    def send(src, dst, ssem, rsem, dev):
        copy(src, dst, ssem, rsem, dev).start()

    def arrived(dst, ssem, rsem):
        copy(dst, dst, ssem, rsem, sibling).wait_recv()

    own_in = pltpu.make_async_copy(x_hbm.at[pl.ds(zl * half, half), :], xa.at[0, c, zl], in_sem.at[0])
    oth_in = pltpu.make_async_copy(x_hbm.at[pl.ds((1 - zl) * half, half), :], ph, in_sem.at[1])
    own_in.start()
    oth_in.start()

    barrier = pltpu.get_barrier_semaphore()
    peers = [sibling]
    peers += [ydev(d) for d in range(1, NY)]
    peers += [xdev(d) for d in range(1, NX)]
    peers += [zdev(d) for d in range(1, NZ)]
    for dev in peers:
        pl.semaphore_signal(barrier, inc=1, device_id=dev, device_id_type=MESH_ID)
    pl.semaphore_wait(barrier, len(peers))

    oth_in.wait()
    own_in.wait()
    send(ph, xa.at[0, c, zl], sw_s, sw_r, {"zl": 1 - zl})

    subs = (zl, 1 - zl)

    def to_minus(k, j):
        t = xa.at[k, c, subs[j]]
        u = xa.at[k + 1, c, subs[j]]
        send(t, u, ring_s, ring_r.at[0, k, j], ydev(-1))

    def to_plus(k, j):
        t = xa.at[(NY - k) % NY, c, subs[j]]
        u = xa.at[NY - k - 1, c, subs[j]]
        send(t, u, ring_s, ring_r.at[1, k, j], ydev(1))

    def to_sibling(k, j):
        t = xa.at[k, c, subs[j]]
        send(t, t, sib_s, sib_r.at[k, j], sibling)

    def from_sibling(k, j):
        arrived(xa.at[k, 1 - c, subs[j]], sib_s, sib_r.at[k, j])

    def partial_margin(g, j):
        off, n = GROUPS[g]
        s = subs[j]
        for p in range(off, off + n):
            k, r = FACTORS[p]
            v = dot(xa[k, 0, s], xa[r, 0, c], (((0,), (0,)), ((), ())))
            v = v + dot(xa[k, 1, s], xa[r, 1, c], (((0,), (0,)), ((), ())))
            v = v.astype(BF16)
            xs[2 * s, p] = v[:xrows]
            xs[2 * s + 1, p] = v[xrows:]
        for i in range(2):
            to = 2 * s + i
            d = lax.rem(to - x + NX, NX)
            at = jnp.maximum(d - 1, 0)
            h = copy(xs.at[to, pl.ds(off, n)], xr.at[at, pl.ds(off, n)], x_s, x_r.at[g], {"x": to})

            @pl.when(d > 0)
            def _():
                h.start()

    def sum_over_x(g):
        off, n = GROUPS[g]
        arrived(xr.at[:, pl.ds(off, n)], x_s, x_r.at[g])
        for p in range(off, off + n):
            v = xs[x, p].astype(F32)
            for d in range(1, NX):
                v = v + xr[d - 1, p].astype(F32)
            zs[:, p] = v.astype(BF16).reshape(NZ, zrows, band)
        for d in range(1, NZ):
            t = lax.rem(z + d, NZ)
            send(
                zs.at[t, pl.ds(off, n)], zr.at[d - 1, pl.ds(off, n)],
                z_s, z_r.at[g], zdev(d),
            )

    def sum_over_z(g):
        off, n = GROUPS[g]
        arrived(zr.at[:, pl.ds(off, n)], z_s, z_r.at[g])
        for p in range(off, off + n):
            v = zs[z, p].astype(F32)
            for d in range(1, NZ):
                v = v + zr[d - 1, p].astype(F32)
            v = v * (1.0 / total_rows)
            if p == 0:
                v = v - unit(zrows, band, x * xrows + z * zrows, c * band)
            w = v.astype(BF16)
            if p == FAR:
                dq[...] = w
                send(dq, db.at[p], q_s, q_r, ydev(-2))
            else:
                d32[p] = v
                db[p] = w
                da[p, z, x] = w

    def place_far():
        arrived(db.at[FAR], q_s, q_r)
        da[FAR, z, x] = db[FAR]

    def unit(rows, cols, row0, col0):
        i = lax.broadcasted_iota(jnp.int32, (rows, cols), 0) + row0
        j = lax.broadcasted_iota(jnp.int32, (rows, cols), 1) + col0
        return (i == j).astype(F32)

    for j in range(2):
        if j == 1:
            arrived(xa.at[0, c, 1 - zl], sw_s, sw_r)
        to_minus(0, j)
        to_plus(0, j)
        to_sibling(0, j)
    def ring_step(h, j):
        if h < 4 or j == 0:
            arrived(xa.at[h, c, subs[j]], ring_s, ring_r.at[0, h - 1, j])
            if h < 3 or (h == 3 and j == 0):
                to_minus(h, j)
            to_sibling(h, j)
        if h < 4 or j == 1:
            arrived(xa.at[NY - h, c, subs[j]], ring_s, ring_r.at[1, h - 1, j])
            if h < 3 or (h == 3 and j == 1):
                to_plus(h, j)
            to_sibling(NY - h, j)

    def gather_x(g):
        off, n = GROUPS[g]
        v = da.at[pl.ds(off, n), z, x]
        for d in range(1, NX):
            send(v, v, gx_s, gx_r.at[g // 4], xdev(d))

    def slab(g, i, h):
        off, n = GROUPS[g]
        t = lax.rem(z + (h if i == 0 else NZ - h), NZ)
        return t, pl.ds(off, n)

    def hop_send(g, i, h):
        t, ps = slab(g, i, h - 1)
        v = da.at[ps, t] if h < 4 else da.at[ps, t, pl.ds(2 * i, 2)]
        send(v, v, gz_s, gz_r.at[g // 4, i, h - 1], zdev(-1 if i == 0 else 1))

    def gather_z(g):
        off, n = GROUPS[g]
        arrived(da.at[pl.ds(off, n), z, pl.ds(0, NX - 1)], gx_s, gx_r.at[g // 4])
        for i in range(2):
            hop_send(g, i, 1)

    def hop(g, h):
        for i in range(2):
            t, ps = slab(g, i, h)
            v = da.at[ps, t] if h < 4 else da.at[ps, t, pl.ds(2 * i, 2)]
            arrived(v, gz_s, gz_r.at[g // 4, i, h - 1])
            if h < 4:
                hop_send(g, i, h + 1)

    def near_z(g):
        off, n = GROUPS[g]
        v = da.at[pl.ds(off, n), z, x]
        for d in range(1, NZ):
            send(db.at[pl.ds(off, n)], v, hz_s, hz_r.at[g - 1, d - 1], zdev(d))

    def pieces_x(g, rs):
        off, n = GROUPS[g]
        for r in rs:
            t = lax.rem(z + r, NZ)
            v = da.at[pl.ds(off, n), t, x]
            if r:
                arrived(v, hz_s, hz_r.at[g - 1, NZ - 1 - r])
            for d in (1, 3, 2):
                send(v if r else db.at[pl.ds(off, n)], v, hp_s, hp_r.at[g - 1], xdev(d))

    def pieces_done(g):
        off, n = GROUPS[g]
        arrived(da.at[pl.ds(off, n), :, pl.ds(0, NX - 1)], hp_s, hp_r.at[g - 1])

    PARTS = ((0, 6), (6, 2))

    def rows_part(i):
        off, n = PARTS[i]
        return pl.ds(off, n)

    def left_send(i):
        ps = rows_part(i)
        for k in range(1, NY):
            send(db.at[ps], dj.at[k, c, ps], y_s, y_r, ydev(-k))
        off, n = PARTS[i]
        for p in range(off, off + n):
            dj[0, c, p] = db[p]
        if i == 1:
            send(db, dj.at[0, c], yf_s, yf_r.at[0], sibling)

    def left_pass():
        v = dj.at[pl.ds(1, NY - 1), c]
        arrived(v, y_s, y_r)
        send(v, v, yf_s, yf_r.at[1], sibling)

    def pair_in(h, j):
        from_sibling(h, j)
        from_sibling(NY - h, j)

    ring_step(1, 0)
    from_sibling(0, 0)
    from_sibling(0, 1)
    partial_margin(0, 0)
    partial_margin(0, 1)
    pair_in(1, 0)
    partial_margin(4, 0)
    ring_step(1, 1)
    pair_in(1, 1)
    partial_margin(4, 1)
    sum_over_x(0)
    ring_step(2, 0)
    pair_in(2, 0)
    partial_margin(1, 0)
    sum_over_z(0)
    gather_x(0)
    ring_step(2, 1)
    sum_over_x(4)
    pair_in(2, 1)
    partial_margin(3, 0)
    partial_margin(3, 1)
    partial_margin(1, 1)
    gather_z(0)
    ring_step(3, 0)
    hop(0, 1)
    sum_over_z(4)
    gather_x(4)
    pair_in(3, 0)
    partial_margin(2, 0)
    sum_over_x(3)
    sum_over_x(1)
    hop(0, 2)
    ring_step(3, 1)
    gather_z(4)
    pair_in(3, 1)
    partial_margin(2, 1)
    sum_over_z(3)
    sum_over_z(1)
    near_z(1)
    pieces_x(1, (0,))
    hop(0, 3)
    hop(4, 1)
    sum_over_x(2)
    place_far()
    near_z(3)
    pieces_x(3, (0,))
    left_send(0)
    ring_step(4, 0)
    ring_step(4, 1)
    hop(0, 4)
    pieces_x(1, (1, 7, 2, 6))
    hop(4, 2)
    pieces_x(1, (3, 5, 4))
    pieces_x(3, (1, 7))
    sum_over_z(2)
    near_z(2)
    pieces_x(2, (0,))
    left_send(1)
    hop(4, 3)
    pieces_x(3, (2, 6, 3, 5, 4))
    pieces_x(2, (1, 7, 2, 6))
    hop(4, 4)
    pieces_x(2, (3, 5, 4))
    left_pass()
    pieces_done(1)
    pieces_done(3)
    pieces_done(2)
    arrived(dj.at[0, 1 - c], yf_s, yf_r.at[0])
    arrived(dj.at[pl.ds(1, NY - 1), 1 - c], yf_s, yf_r.at[1])

    def piece(b, t, u):
        off, n = HALVES[b]
        return ca.at[t, u, pl.ds(off, n)]

    def zpiece(b, u, i, h, far):
        off, n = HALVES[b]
        first = (n + 1) // 2
        t = lax.rem(z + (h if i == 0 else NZ - h), NZ)
        if not far:
            return piece(b, t, u)
        return ca.at[t, u, pl.ds(off, first) if i == 0 else pl.ds(off + first, n - first)]

    def a_send(d, i, h):
        v = zpiece(0, lax.rem(x + NX - d, NX), i, h - 1, h == 4)
        send(v, v, az_s, az_r.at[d, i, h - 1], zdev(-1 if i == 0 else 1))

    def a_hop(d, h):
        for i in range(2):
            v = zpiece(0, lax.rem(x + NX - d, NX), i, h, h == 4)
            arrived(v, az_s, az_r.at[d, i, h - 1])
            if h < 4:
                a_send(d, i, h + 1)

    def b_send(i, h):
        v = zpiece(1, x, i, h - 1, h == 4)
        send(v, v, bz_s, bz_r.at[i, h - 1], zdev(-1 if i == 0 else 1))

    def b_along_x(r):
        v = piece(1, lax.rem(z + r, NZ), x)
        for d in (1, 3, 2):
            send(v, v, bx_s, bx_r, xdev(d))

    def b_hop(h):
        for i in range(2):
            arrived(zpiece(1, x, i, h, h == 4), bz_s, bz_r.at[i, h - 1])
            if h < 4:
                b_send(i, h + 1)
        if h < 4:
            b_along_x(h)
            b_along_x(NZ - h)
        else:
            b_along_x(4)

    def plane_gather(between, b_done):
        for d in (1, 3, 2):
            send(piece(0, z, x), piece(0, z, x), ax_s, ax_r.at[d - 1], xdev(d))
        for i in range(2):
            b_send(i, 1)
        for i in range(2):
            a_send(0, i, 1)
        b_along_x(0)
        b_hop(1)
        for d in (1, 3, 2):
            u = lax.rem(x + NX - d, NX)
            arrived(piece(0, z, u), ax_s, ax_r.at[d - 1])
            for i in range(2):
                a_send(d, i, 1)
        a_hop(0, 1)
        between()
        for h in range(2, 6):
            if h < 5:
                b_hop(h)
            else:
                arrived(ca.at[:, pl.ds(0, NX - 1), pl.ds(*HALVES[1])], bx_s, bx_r)
                b_done()
            for d in (1, 3, 2):
                a_hop(d, h - 1)
            if h < 5:
                a_hop(0, h)

    def rows_of(p, s):
        return jnp.concatenate([ca[:, 2 * s + i, p].reshape(xrows, band) for i in range(2)], axis=0)

    def dev_rows(p, s):
        return jnp.concatenate([da[p, :, 2 * s + i].reshape(xrows, band) for i in range(2)], axis=0)

    acc_sq = [None] * NY
    for k in range(NY):
        left = [dj[k, s].reshape(NY * zrows, band) for s in range(2)]
        part = dot(left[0], dev_rows(POS[k], 0)) + dot(left[1], dev_rows(POS[k], 1))
        for p in range(NY):
            m = POS[(k + SLOT[p]) % NY]
            rows = part[p * zrows : (p + 1) * zrows]
            acc_sq[m] = rows if acc_sq[m] is None else acc_sq[m] + rows
    for p in range(NY):
        v = 0.375 * acc_sq[p] - 0.5 * (db[p].astype(F32) if p == FAR else d32[p])
        if p == 0:
            v = v + unit(zrows, band, x * xrows + z * zrows, c * band)
        ca[z, x, p] = v.astype(BF16)

    kg = lax.rem(x * 2 + zh // 2 - y + NY, NY)
    near = jnp.where(kg == 0, 0, jnp.where(kg <= 2, 2 * kg - 1, 2 * (NY - kg)))
    pg = jnp.where(kg == 3, 6, jnp.where(kg == 4, FAR, jnp.where(kg == 5, 7, near)))

    def mirror(core):
        q = lax.rem(zh, 2) * 2 + core
        return da[pg, :, q].reshape(xrows, band).astype(F32)

    def margin_work():
        from_sibling(4, 0)
        from_sibling(4, 1)
        ms[...] = mirror(1 - c).astype(BF16)
        send(ms, mr, m_s, m_r, sibling)

    home = zl == c
    kept = pl.ds(pl.multiple_of(zl * half, half), half)
    swapped = pl.ds(pl.multiple_of((1 - zl) * half, half), half)
    to_pair = {"zl": 1 - zl}

    def product(part):
        for i, cc in enumerate((1 - c, c)):
            tile = half // 2
            for m in range(2):
                rows = pl.ds(m * tile, tile)
                v = None
                for p in range(HALVES[part][0], sum(HALVES[part])):
                    for s in range(2):
                        w = dot(xa[SLOT[p], cc, s, rows], rows_of(p, s))
                        v = w if v is None else v + w
                acc[i, rows] = v if part == 1 else acc[i, rows] + v
            if part == 0:
                osb[i] = acc[i].astype(BF16)
                if i == 0:
                    copy(osb.at[0], rb, os_s, os_r, sibling).start()
                else:

                    @pl.when(home)
                    def _():
                        o_out[kept, :] = osb[1]

                    @pl.when(jnp.logical_not(home))
                    def _():
                        copy(osb.at[1], land, oz_s, oz_r, to_pair).start()

    def first_half():
        arrived(mr, m_s, m_r)
        v = jnp.where(zl == c, mirror(c), mr[...].astype(F32))
        rows0 = (y * 2 + zl) * band
        cols0 = (x * 8 + zh * 2 + c) * xrows
        m_out[...] = v.T + unit(band, xrows, rows0, cols0)
        product(1)

    plane_gather(margin_work, first_half)

    @pl.when(home)
    def _():
        arrived(rb, os_s, os_r)
        copy(rb, land, oz_s, oz_r, to_pair).start()

    product(0)

    low = pl.ds(0, NZ - 1)
    three = pl.ds(0, NX - 1)
    for v, sem in (
        (ph, sw_s),
        (xa.at[pl.ds(0, 7), :, 0], ring_s),
        (xa.at[:, :, 0], sib_s),
        (xr, x_s),
        (zr, z_s),
        (dq, q_s),
        (dj.at[pl.ds(1, NY - 1), 0], y_s),
        (dj.at[:, 0], yf_s),
        (da.at[three, 0, three], gx_s),
        (da.at[three, low], gz_s),
        (da.at[pl.ds(0, 5), low, 0], hz_s),
        (da.at[pl.ds(0, 5), :, three], hp_s),
        (ca.at[0, three, pl.ds(*HALVES[0])], ax_s),
        (ca.at[low, :, pl.ds(*HALVES[0])], az_s),
        (ca.at[low, 0, pl.ds(*HALVES[1])], bz_s),
        (ca.at[:, three, pl.ds(*HALVES[1])], bx_s),
        (ms, m_s),
    ):
        copy(v, v, sem, m_r, sibling).wait_send()

    @pl.when(jnp.logical_not(home))
    def _():
        arrived(rb, os_s, os_r)
        o_out[kept, :] = rb[...]

    arrived(land, oz_s, oz_r)
    o_out[swapped, :] = land[...]

    copy(rb, rb, os_s, os_r, sibling).wait_send()
    copy(rb, rb, oz_s, oz_r, sibling).wait_send()


def shards(total_rows, orbitals):
    rows, band = orbitals.shape
    half = rows // 2
    xrows = 2 * band // NX
    zrows = xrows // NZ
    dma = pltpu.SemaphoreType.DMA
    v = pltpu.VMEM
    scratch = [
        v((NY, 2, 2, half, band), BF16),
        v((half, band), BF16),
        v((NX, NY, xrows, band), BF16),
        v((NX - 1, NY, xrows, band), BF16),
        v((NZ, NY, zrows, band), BF16),
        v((NZ - 1, NY, zrows, band), BF16),
        v((NY, zrows, band), BF16),
        v((NY, zrows, band), F32),
        v((zrows, band), BF16),
        v((NY, 2, NY, zrows, band), BF16),
        v((NY, NZ, NX, zrows, band), BF16),
        v((NZ, NX, NY, zrows, band), BF16),
        v((xrows, band), BF16),
        v((xrows, band), BF16),
        v((2, half, band), F32),
        v((2, half, band), BF16),
        v((half, band), BF16),
        v((half, band), BF16),
        dma((2,)),
        dma, dma,
        dma, dma((2, 4, 2)),
        dma, dma((NY, 2)),
        dma, dma((5,)),
        dma, dma((5,)),
        dma, dma,
        dma, dma,
        dma, dma((2,)),
        dma, dma((2,)),
        dma, dma((2, 2, 4)),
        dma, dma((3, NZ - 1)),
        dma, dma((3,)),
        dma, dma((NX - 1,)),
        dma, dma((NX, 2, 4)),
        dma, dma((2, 4)),
        dma, dma,
        dma, dma,
        dma, dma,
        dma, dma,
    ]

    def body(*refs):
        kernel(total_rows, *refs)

    margin, corrected = pl.pallas_call(
        body,
        out_shape=(v((band, xrows), F32), v((rows, band), BF16)),
        in_specs=[pl.BlockSpec(memory_space=pl.ANY)],
        out_specs=(pl.BlockSpec(memory_space=pltpu.VMEM), pl.BlockSpec(memory_space=pltpu.VMEM)),
        scratch_shapes=scratch,
        compiler_params=pltpu.CompilerParams(
            collective_id=0, has_side_effects=True, vmem_limit_bytes=56 * 1024 * 1024
        ),
    )(orbitals)
    return pl.pallas_call(
        write_out,
        out_shape=(
            jax.ShapeDtypeStruct((band, xrows), F32),
            jax.ShapeDtypeStruct((rows, band), BF16),
        ),
        in_specs=[pl.BlockSpec(memory_space=pltpu.VMEM)] * 2,
        out_specs=(pl.BlockSpec(memory_space=pl.ANY),) * 2,
        scratch_shapes=[dma((2,))],
        compiler_params=pltpu.CompilerParams(vmem_limit_bytes=4 * 1024 * 1024),
    )(margin, corrected)


def write_out(m_ref, o_ref, m_out, o_out, sem):
    copies = [
        pltpu.make_async_copy(m_ref, m_out, sem.at[0]),
        pltpu.make_async_copy(o_ref, o_out, sem.at[1]),
    ]
    for h in copies:
        h.start()
    for h in copies:
        h.wait()


def solution(mesh):
    finer = Mesh(mesh.devices.reshape(NY, 2, NX, NZ // 2, 2), AXES)
    coeffs = ("x", "zh", "c")
    bands = ("y", "zl")

    def run(orbitals):
        total = orbitals.shape[0]
        return jax.shard_map(
            lambda o: shards(total, o),
            mesh=finer,
            in_specs=(P(coeffs, bands),),
            out_specs=(P(bands, coeffs), P(coeffs, bands)),
            check_vma=False,
        )(orbitals)

    return run
```

```python
import jax
import jax.numpy as jnp
from jax import lax
from jax.experimental import pallas as pl
from jax.experimental.pallas import tpu as pltpu
from jax.sharding import Mesh
from jax.sharding import PartitionSpec as P

AXES = ("y", "zl", "x", "zh", "c")
NY, NX, NZ = 8, 4, 8
SLOT = (0, 1, 7, 2, 6, 4, 3, 5)
POS = tuple(SLOT.index(k) for k in range(NY))
GROUPS = ((0, 1), (3, 2), (6, 2), (5, 1), (1, 2))
FACTORS = ((0, 0), (1, 0), (7, 0), (2, 0), (6, 0), (2, 6), (3, 0), (5, 0))
FAR = 5
HALVES = ((0, 3), (3, 5))
MESH_ID = pl.DeviceIdType.MESH
F32 = jnp.float32
BF16 = jnp.bfloat16


def dot(a, b, dims=(((1,), (0,)), ((), ()))):
    return lax.dot_general(a, b, dims, preferred_element_type=F32)


def kernel(
    total_rows, x_hbm, m_out, o_out, xa, ph, xs, xr, zs, zr, db, d32, dq, dj, da, ca,
    ms, mr, acc, osb, rb, land, in_sem, sw_s, sw_r, ring_s, ring_r, sib_s, sib_r, x_s, x_r, z_s, z_r,
    q_s, q_r, y_s, y_r, yf_s, yf_r, gx_s, gx_r, gz_s, gz_r, hz_s, hz_r, hp_s, hp_r,
    ax_s, ax_r, az_s, az_r, bz_s, bz_r, bx_s, bx_r, m_s, m_r, os_s, os_r, oz_s, oz_r,
):
    y = lax.axis_index("y")
    zl = lax.axis_index("zl")
    x = lax.axis_index("x")
    zh = lax.axis_index("zh")
    c = lax.axis_index("c")
    z = zh * 2 + zl
    half = ph.shape[0]
    band = ph.shape[1]
    xrows = xs.shape[2]
    zrows = zs.shape[2]

    def zdev(d):
        t = lax.rem(z + d + NZ, NZ)
        return {"zh": t // 2, "zl": lax.rem(t, 2)}

    def ydev(d):
        return {"y": lax.rem(y + d + NY, NY)}

    def xdev(d):
        return {"x": lax.rem(x + d + NX, NX)}

    sibling = {"c": 1 - c}

    def copy(src, dst, ssem, rsem, dev):
        return pltpu.make_async_remote_copy(
            src_ref=src, dst_ref=dst, send_sem=ssem, recv_sem=rsem, device_id=dev, device_id_type=MESH_ID
        )

    def send(src, dst, ssem, rsem, dev):
        copy(src, dst, ssem, rsem, dev).start()

    def arrived(dst, ssem, rsem):
        copy(dst, dst, ssem, rsem, sibling).wait_recv()

    own_in = pltpu.make_async_copy(x_hbm.at[pl.ds(zl * half, half), :], xa.at[0, c, zl], in_sem.at[0])
    oth_in = pltpu.make_async_copy(x_hbm.at[pl.ds((1 - zl) * half, half), :], ph, in_sem.at[1])
    own_in.start()
    oth_in.start()

    barrier = pltpu.get_barrier_semaphore()
    peers = [sibling]
    peers += [ydev(d) for d in range(1, NY)]
    peers += [xdev(d) for d in range(1, NX)]
    peers += [zdev(d) for d in range(1, NZ)]
    for dev in peers:
        pl.semaphore_signal(barrier, inc=1, device_id=dev, device_id_type=MESH_ID)
    pl.semaphore_wait(barrier, len(peers))

    oth_in.wait()
    own_in.wait()
    send(ph, xa.at[0, c, zl], sw_s, sw_r, {"zl": 1 - zl})

    subs = (zl, 1 - zl)

    def to_minus(k, j):
        t = xa.at[k, c, subs[j]]
        u = xa.at[k + 1, c, subs[j]]
        send(t, u, ring_s, ring_r.at[0, k, j], ydev(-1))

    def to_plus(k, j):
        t = xa.at[(NY - k) % NY, c, subs[j]]
        u = xa.at[NY - k - 1, c, subs[j]]
        send(t, u, ring_s, ring_r.at[1, k, j], ydev(1))

    def to_sibling(k, j):
        t = xa.at[k, c, subs[j]]
        send(t, t, sib_s, sib_r.at[k, j], sibling)

    def from_sibling(k, j):
        arrived(xa.at[k, 1 - c, subs[j]], sib_s, sib_r.at[k, j])

    def partial_margin(g, j):
        off, n = GROUPS[g]
        s = subs[j]
        for p in range(off, off + n):
            k, r = FACTORS[p]
            v = dot(xa[k, 0, s], xa[r, 0, c], (((0,), (0,)), ((), ())))
            v = v + dot(xa[k, 1, s], xa[r, 1, c], (((0,), (0,)), ((), ())))
            v = v.astype(BF16)
            xs[2 * s, p] = v[:xrows]
            xs[2 * s + 1, p] = v[xrows:]
        for i in range(2):
            to = 2 * s + i
            d = lax.rem(to - x + NX, NX)
            at = jnp.maximum(d - 1, 0)
            h = copy(xs.at[to, pl.ds(off, n)], xr.at[at, pl.ds(off, n)], x_s, x_r.at[g], {"x": to})

            @pl.when(d > 0)
            def _():
                h.start()

    def sum_over_x(g):
        off, n = GROUPS[g]
        arrived(xr.at[:, pl.ds(off, n)], x_s, x_r.at[g])
        for p in range(off, off + n):
            v = xs[x, p].astype(F32)
            for d in range(1, NX):
                v = v + xr[d - 1, p].astype(F32)
            zs[:, p] = v.astype(BF16).reshape(NZ, zrows, band)
        for d in range(1, NZ):
            t = lax.rem(z + d, NZ)
            send(
                zs.at[t, pl.ds(off, n)], zr.at[d - 1, pl.ds(off, n)],
                z_s, z_r.at[g], zdev(d),
            )

    def sum_over_z(g):
        off, n = GROUPS[g]
        arrived(zr.at[:, pl.ds(off, n)], z_s, z_r.at[g])
        for p in range(off, off + n):
            v = zs[z, p].astype(F32)
            for d in range(1, NZ):
                v = v + zr[d - 1, p].astype(F32)
            v = v * (1.0 / total_rows)
            if p == 0:
                v = v - unit(zrows, band, x * xrows + z * zrows, c * band)
            w = v.astype(BF16)
            if p == FAR:
                dq[...] = w
                send(dq, db.at[p], q_s, q_r, ydev(-2))
            else:
                d32[p] = v
                db[p] = w
                da[p, z, x] = w

    def place_far():
        arrived(db.at[FAR], q_s, q_r)
        da[FAR, z, x] = db[FAR]

    def unit(rows, cols, row0, col0):
        i = lax.broadcasted_iota(jnp.int32, (rows, cols), 0) + row0
        j = lax.broadcasted_iota(jnp.int32, (rows, cols), 1) + col0
        return (i == j).astype(F32)

    for j in range(2):
        if j == 1:
            arrived(xa.at[0, c, 1 - zl], sw_s, sw_r)
        to_minus(0, j)
        to_plus(0, j)
        to_sibling(0, j)
    def ring_step(h, j):
        if h < 4 or j == 0:
            arrived(xa.at[h, c, subs[j]], ring_s, ring_r.at[0, h - 1, j])
            if h < 3 or (h == 3 and j == 0):
                to_minus(h, j)
            to_sibling(h, j)
        if h < 4 or j == 1:
            arrived(xa.at[NY - h, c, subs[j]], ring_s, ring_r.at[1, h - 1, j])
            if h < 3 or (h == 3 and j == 1):
                to_plus(h, j)
            to_sibling(NY - h, j)

    def gather_x(g):
        off, n = GROUPS[g]
        v = da.at[pl.ds(off, n), z, x]
        for d in range(1, NX):
            send(v, v, gx_s, gx_r.at[g // 4], xdev(d))

    def slab(g, i, h):
        off, n = GROUPS[g]
        t = lax.rem(z + (h if i == 0 else NZ - h), NZ)
        return t, pl.ds(off, n)

    def hop_send(g, i, h):
        t, ps = slab(g, i, h - 1)
        v = da.at[ps, t] if h < 4 else da.at[ps, t, pl.ds(2 * i, 2)]
        send(v, v, gz_s, gz_r.at[g // 4, i, h - 1], zdev(-1 if i == 0 else 1))

    def gather_z(g):
        off, n = GROUPS[g]
        arrived(da.at[pl.ds(off, n), z, pl.ds(0, NX - 1)], gx_s, gx_r.at[g // 4])
        for i in range(2):
            hop_send(g, i, 1)

    def hop(g, h):
        for i in range(2):
            t, ps = slab(g, i, h)
            v = da.at[ps, t] if h < 4 else da.at[ps, t, pl.ds(2 * i, 2)]
            arrived(v, gz_s, gz_r.at[g // 4, i, h - 1])
            if h < 4:
                hop_send(g, i, h + 1)

    def near_z(g):
        off, n = GROUPS[g]
        v = da.at[pl.ds(off, n), z, x]
        for d in range(1, NZ):
            send(db.at[pl.ds(off, n)], v, hz_s, hz_r.at[g - 1, d - 1], zdev(d))

    def pieces_x(g, rs):
        off, n = GROUPS[g]
        for r in rs:
            t = lax.rem(z + r, NZ)
            v = da.at[pl.ds(off, n), t, x]
            if r:
                arrived(v, hz_s, hz_r.at[g - 1, NZ - 1 - r])
            for d in (1, 3, 2):
                send(v if r else db.at[pl.ds(off, n)], v, hp_s, hp_r.at[g - 1], xdev(d))

    def pieces_done(g):
        off, n = GROUPS[g]
        arrived(da.at[pl.ds(off, n), :, pl.ds(0, NX - 1)], hp_s, hp_r.at[g - 1])

    PARTS = ((0, 6), (6, 2))

    def rows_part(i):
        off, n = PARTS[i]
        return pl.ds(off, n)

    def left_send(i):
        ps = rows_part(i)
        for k in range(1, NY):
            send(db.at[ps], dj.at[k, c, ps], y_s, y_r, ydev(-k))
        off, n = PARTS[i]
        for p in range(off, off + n):
            dj[0, c, p] = db[p]
        if i == 1:
            send(db, dj.at[0, c], yf_s, yf_r.at[0], sibling)

    def left_pass():
        v = dj.at[pl.ds(1, NY - 1), c]
        arrived(v, y_s, y_r)
        send(v, v, yf_s, yf_r.at[1], sibling)

    def pair_in(h, j):
        from_sibling(h, j)
        from_sibling(NY - h, j)

    ring_step(1, 0)
    from_sibling(0, 0)
    from_sibling(0, 1)
    partial_margin(0, 0)
    partial_margin(0, 1)
    pair_in(1, 0)
    partial_margin(4, 0)
    ring_step(1, 1)
    pair_in(1, 1)
    partial_margin(4, 1)
    sum_over_x(0)
    ring_step(2, 0)
    pair_in(2, 0)
    partial_margin(1, 0)
    sum_over_z(0)
    gather_x(0)
    ring_step(2, 1)
    sum_over_x(4)
    pair_in(2, 1)
    partial_margin(3, 0)
    partial_margin(3, 1)
    partial_margin(1, 1)
    gather_z(0)
    ring_step(3, 0)
    hop(0, 1)
    sum_over_z(4)
    gather_x(4)
    pair_in(3, 0)
    partial_margin(2, 0)
    sum_over_x(3)
    sum_over_x(1)
    hop(0, 2)
    ring_step(3, 1)
    gather_z(4)
    pair_in(3, 1)
    partial_margin(2, 1)
    sum_over_z(3)
    sum_over_z(1)
    near_z(1)
    pieces_x(1, (0,))
    hop(0, 3)
    hop(4, 1)
    sum_over_x(2)
    place_far()
    near_z(3)
    pieces_x(3, (0,))
    left_send(0)
    ring_step(4, 0)
    ring_step(4, 1)
    pieces_x(1, (1, 7, 2, 6))
    hop(4, 2)
    pieces_x(1, (3, 5, 4))
    sum_over_z(2)
    near_z(2)
    pieces_x(2, (0,))
    left_send(1)
    pieces_x(3, (1, 7, 2, 6))
    hop(4, 3)
    pieces_x(3, (3, 5, 4))
    pieces_x(2, (1, 7, 2, 6, 3, 5, 4))
    hop(0, 4)
    hop(4, 4)
    left_pass()
    pieces_done(1)
    pieces_done(3)
    arrived(dj.at[0, 1 - c], yf_s, yf_r.at[0])
    arrived(dj.at[pl.ds(1, NY - 1), 1 - c], yf_s, yf_r.at[1])

    def piece(b, t, u):
        off, n = HALVES[b]
        return ca.at[t, u, pl.ds(off, n)]

    def zpiece(b, u, i, h, far):
        off, n = HALVES[b]
        first = (n + 1) // 2
        t = lax.rem(z + (h if i == 0 else NZ - h), NZ)
        if not far:
            return piece(b, t, u)
        return ca.at[t, u, pl.ds(off, first) if i == 0 else pl.ds(off + first, n - first)]

    def a_send(d, i, h):
        v = zpiece(0, lax.rem(x + NX - d, NX), i, h - 1, h == 4)
        send(v, v, az_s, az_r.at[d, i, h - 1], zdev(-1 if i == 0 else 1))

    def a_hop(d, h):
        for i in range(2):
            v = zpiece(0, lax.rem(x + NX - d, NX), i, h, h == 4)
            arrived(v, az_s, az_r.at[d, i, h - 1])
            if h < 4:
                a_send(d, i, h + 1)

    def b_send(i, h):
        v = zpiece(1, x, i, h - 1, h == 4)
        send(v, v, bz_s, bz_r.at[i, h - 1], zdev(-1 if i == 0 else 1))

    def b_along_x(r):
        v = piece(1, lax.rem(z + r, NZ), x)
        for d in (1, 3, 2):
            send(v, v, bx_s, bx_r, xdev(d))

    def b_hop(h):
        for i in range(2):
            arrived(zpiece(1, x, i, h, h == 4), bz_s, bz_r.at[i, h - 1])
            if h < 4:
                b_send(i, h + 1)
        if h < 4:
            b_along_x(h)
            b_along_x(NZ - h)
        else:
            b_along_x(4)

    def plane_gather(between, b_done):
        for d in (1, 3, 2):
            send(piece(0, z, x), piece(0, z, x), ax_s, ax_r.at[d - 1], xdev(d))
        for i in range(2):
            b_send(i, 1)
        for i in range(2):
            a_send(0, i, 1)
        b_along_x(0)
        b_hop(1)
        for d in (1, 3, 2):
            u = lax.rem(x + NX - d, NX)
            arrived(piece(0, z, u), ax_s, ax_r.at[d - 1])
            for i in range(2):
                a_send(d, i, 1)
        a_hop(0, 1)
        between()
        for h in range(2, 6):
            if h < 5:
                b_hop(h)
            else:
                arrived(ca.at[:, pl.ds(0, NX - 1), pl.ds(*HALVES[1])], bx_s, bx_r)
                b_done()
            for d in (1, 3, 2):
                a_hop(d, h - 1)
            if h < 5:
                a_hop(0, h)

    def rows_of(p, s):
        return jnp.concatenate([ca[:, 2 * s + i, p].reshape(xrows, band) for i in range(2)], axis=0)

    def dev_rows(p, s):
        return jnp.concatenate([da[p, :, 2 * s + i].reshape(xrows, band) for i in range(2)], axis=0)

    acc_sq = [None] * NY
    for k in SLOT:
        if POS[k] == GROUPS[2][0]:
            pieces_done(2)
        left = [dj[k, s].reshape(NY * zrows, band) for s in range(2)]
        part = dot(left[0], dev_rows(POS[k], 0)) + dot(left[1], dev_rows(POS[k], 1))
        for p in range(NY):
            m = POS[(k + SLOT[p]) % NY]
            rows = part[p * zrows : (p + 1) * zrows]
            acc_sq[m] = rows if acc_sq[m] is None else acc_sq[m] + rows
    for p in range(NY):
        v = 0.375 * acc_sq[p] - 0.5 * (db[p].astype(F32) if p == FAR else d32[p])
        if p == 0:
            v = v + unit(zrows, band, x * xrows + z * zrows, c * band)
        ca[z, x, p] = v.astype(BF16)

    kg = lax.rem(x * 2 + zh // 2 - y + NY, NY)
    near = jnp.where(kg == 0, 0, jnp.where(kg <= 2, 2 * kg - 1, 2 * (NY - kg)))
    pg = jnp.where(kg == 3, 6, jnp.where(kg == 4, FAR, jnp.where(kg == 5, 7, near)))

    def mirror(core):
        q = lax.rem(zh, 2) * 2 + core
        return da[pg, :, q].reshape(xrows, band).astype(F32)

    def margin_work():
        from_sibling(4, 0)
        from_sibling(4, 1)
        ms[...] = mirror(1 - c).astype(BF16)
        send(ms, mr, m_s, m_r, sibling)

    home = zl == c
    kept = pl.ds(pl.multiple_of(zl * half, half), half)
    swapped = pl.ds(pl.multiple_of((1 - zl) * half, half), half)
    to_pair = {"zl": 1 - zl}

    def product(part):
        for i, cc in enumerate((1 - c, c)):
            tile = half // 2
            for m in range(2):
                rows = pl.ds(m * tile, tile)
                v = None
                for p in range(HALVES[part][0], sum(HALVES[part])):
                    for s in range(2):
                        w = dot(xa[SLOT[p], cc, s, rows], rows_of(p, s))
                        v = w if v is None else v + w
                acc[i, rows] = v if part == 1 else acc[i, rows] + v
            if part == 0:
                osb[i] = acc[i].astype(BF16)
                if i == 0:
                    copy(osb.at[0], rb, os_s, os_r, sibling).start()
                else:

                    @pl.when(home)
                    def _():
                        o_out[kept, :] = osb[1]

                    @pl.when(jnp.logical_not(home))
                    def _():
                        copy(osb.at[1], land, oz_s, oz_r, to_pair).start()

    def first_half():
        arrived(mr, m_s, m_r)
        v = jnp.where(zl == c, mirror(c), mr[...].astype(F32))
        rows0 = (y * 2 + zl) * band
        cols0 = (x * 8 + zh * 2 + c) * xrows
        m_out[...] = v.T + unit(band, xrows, rows0, cols0)
        product(1)

    plane_gather(margin_work, first_half)

    @pl.when(home)
    def _():
        arrived(rb, os_s, os_r)
        copy(rb, land, oz_s, oz_r, to_pair).start()

    product(0)

    low = pl.ds(0, NZ - 1)
    three = pl.ds(0, NX - 1)
    for v, sem in (
        (ph, sw_s),
        (xa.at[pl.ds(0, 7), :, 0], ring_s),
        (xa.at[:, :, 0], sib_s),
        (xr, x_s),
        (zr, z_s),
        (dq, q_s),
        (dj.at[pl.ds(1, NY - 1), 0], y_s),
        (dj.at[:, 0], yf_s),
        (da.at[three, 0, three], gx_s),
        (da.at[three, low], gz_s),
        (da.at[pl.ds(0, 5), low, 0], hz_s),
        (da.at[pl.ds(0, 5), :, three], hp_s),
        (ca.at[0, three, pl.ds(*HALVES[0])], ax_s),
        (ca.at[low, :, pl.ds(*HALVES[0])], az_s),
        (ca.at[low, 0, pl.ds(*HALVES[1])], bz_s),
        (ca.at[:, three, pl.ds(*HALVES[1])], bx_s),
        (ms, m_s),
    ):
        copy(v, v, sem, m_r, sibling).wait_send()

    @pl.when(jnp.logical_not(home))
    def _():
        arrived(rb, os_s, os_r)
        o_out[kept, :] = rb[...]

    arrived(land, oz_s, oz_r)
    o_out[swapped, :] = land[...]

    copy(rb, rb, os_s, os_r, sibling).wait_send()
    copy(rb, rb, oz_s, oz_r, sibling).wait_send()


def shards(total_rows, orbitals):
    rows, band = orbitals.shape
    half = rows // 2
    xrows = 2 * band // NX
    zrows = xrows // NZ
    dma = pltpu.SemaphoreType.DMA
    v = pltpu.VMEM
    scratch = [
        v((NY, 2, 2, half, band), BF16),
        v((half, band), BF16),
        v((NX, NY, xrows, band), BF16),
        v((NX - 1, NY, xrows, band), BF16),
        v((NZ, NY, zrows, band), BF16),
        v((NZ - 1, NY, zrows, band), BF16),
        v((NY, zrows, band), BF16),
        v((NY, zrows, band), F32),
        v((zrows, band), BF16),
        v((NY, 2, NY, zrows, band), BF16),
        v((NY, NZ, NX, zrows, band), BF16),
        v((NZ, NX, NY, zrows, band), BF16),
        v((xrows, band), BF16),
        v((xrows, band), BF16),
        v((2, half, band), F32),
        v((2, half, band), BF16),
        v((half, band), BF16),
        v((half, band), BF16),
        dma((2,)),
        dma, dma,
        dma, dma((2, 4, 2)),
        dma, dma((NY, 2)),
        dma, dma((5,)),
        dma, dma((5,)),
        dma, dma,
        dma, dma,
        dma, dma((2,)),
        dma, dma((2,)),
        dma, dma((2, 2, 4)),
        dma, dma((3, NZ - 1)),
        dma, dma((3,)),
        dma, dma((NX - 1,)),
        dma, dma((NX, 2, 4)),
        dma, dma((2, 4)),
        dma, dma,
        dma, dma,
        dma, dma,
        dma, dma,
    ]

    def body(*refs):
        kernel(total_rows, *refs)

    margin, corrected = pl.pallas_call(
        body,
        out_shape=(v((band, xrows), F32), v((rows, band), BF16)),
        in_specs=[pl.BlockSpec(memory_space=pl.ANY)],
        out_specs=(pl.BlockSpec(memory_space=pltpu.VMEM), pl.BlockSpec(memory_space=pltpu.VMEM)),
        scratch_shapes=scratch,
        compiler_params=pltpu.CompilerParams(
            collective_id=0, has_side_effects=True, vmem_limit_bytes=56 * 1024 * 1024
        ),
    )(orbitals)
    return pl.pallas_call(
        write_out,
        out_shape=(
            jax.ShapeDtypeStruct((band, xrows), F32),
            jax.ShapeDtypeStruct((rows, band), BF16),
        ),
        in_specs=[pl.BlockSpec(memory_space=pltpu.VMEM)] * 2,
        out_specs=(pl.BlockSpec(memory_space=pl.ANY),) * 2,
        scratch_shapes=[dma((2,))],
        compiler_params=pltpu.CompilerParams(vmem_limit_bytes=4 * 1024 * 1024),
    )(margin, corrected)


def write_out(m_ref, o_ref, m_out, o_out, sem):
    copies = [
        pltpu.make_async_copy(m_ref, m_out, sem.at[0]),
        pltpu.make_async_copy(o_ref, o_out, sem.at[1]),
    ]
    for h in copies:
        h.start()
    for h in copies:
        h.wait()


def solution(mesh):
    finer = Mesh(mesh.devices.reshape(NY, 2, NX, NZ // 2, 2), AXES)
    coeffs = ("x", "zh", "c")
    bands = ("y", "zl")

    def run(orbitals):
        total = orbitals.shape[0]
        return jax.shard_map(
            lambda o: shards(total, o),
            mesh=finer,
            in_specs=(P(coeffs, bands),),
            out_specs=(P(bands, coeffs), P(coeffs, bands)),
            check_vma=False,
        )(orbitals)

    return run
```

```python
import jax
import jax.numpy as jnp
from jax import lax
from jax.experimental import pallas as pl
from jax.experimental.pallas import tpu as pltpu
from jax.sharding import Mesh
from jax.sharding import PartitionSpec as P

AXES = ("y", "zl", "x", "zh", "c")
NY, NX, NZ = 8, 4, 8
SLOT = (0, 1, 7, 2, 6, 4, 3, 5)
POS = tuple(SLOT.index(k) for k in range(NY))
GROUPS = ((0, 1), (3, 2), (6, 2), (5, 1), (1, 2))
FACTORS = ((0, 0), (1, 0), (7, 0), (2, 0), (6, 0), (2, 6), (3, 0), (5, 0))
FAR = 5
HALVES = ((0, 3), (3, 5))
MESH_ID = pl.DeviceIdType.MESH
F32 = jnp.float32
BF16 = jnp.bfloat16


def dot(a, b, dims=(((1,), (0,)), ((), ()))):
    return lax.dot_general(a, b, dims, preferred_element_type=F32)


def kernel(
    total_rows, x_hbm, m_out, o_out, xa, ph, xs, xr, zs, zr, db, d32, dq, dj, da, ca,
    ms, mr, acc, osb, rb, land, in_sem, sw_s, sw_r, ring_s, ring_r, sib_s, sib_r, x_s, x_r, z_s, z_r,
    q_s, q_r, y_s, y_r, yf_s, yf_r, gx_s, gx_r, gz_s, gz_r, hz_s, hz_r, hp_s, hp_r,
    ax_s, ax_r, az_s, az_r, bz_s, bz_r, bx_s, bx_r, m_s, m_r, os_s, os_r, oz_s, oz_r,
):
    y = lax.axis_index("y")
    zl = lax.axis_index("zl")
    x = lax.axis_index("x")
    zh = lax.axis_index("zh")
    c = lax.axis_index("c")
    z = zh * 2 + zl
    half = ph.shape[0]
    band = ph.shape[1]
    xrows = xs.shape[2]
    zrows = zs.shape[2]

    def zdev(d):
        t = lax.rem(z + d + NZ, NZ)
        return {"zh": t // 2, "zl": lax.rem(t, 2)}

    def ydev(d):
        return {"y": lax.rem(y + d + NY, NY)}

    def xdev(d):
        return {"x": lax.rem(x + d + NX, NX)}

    sibling = {"c": 1 - c}

    def copy(src, dst, ssem, rsem, dev):
        return pltpu.make_async_remote_copy(
            src_ref=src, dst_ref=dst, send_sem=ssem, recv_sem=rsem, device_id=dev, device_id_type=MESH_ID
        )

    def send(src, dst, ssem, rsem, dev):
        copy(src, dst, ssem, rsem, dev).start()

    def arrived(dst, ssem, rsem):
        copy(dst, dst, ssem, rsem, sibling).wait_recv()

    own_in = pltpu.make_async_copy(x_hbm.at[pl.ds(zl * half, half), :], xa.at[0, c, zl], in_sem.at[0])
    oth_in = pltpu.make_async_copy(x_hbm.at[pl.ds((1 - zl) * half, half), :], ph, in_sem.at[1])
    own_in.start()
    oth_in.start()

    barrier = pltpu.get_barrier_semaphore()
    peers = [sibling]
    peers += [ydev(d) for d in range(1, NY)]
    peers += [xdev(d) for d in range(1, NX)]
    peers += [zdev(d) for d in range(1, NZ)]
    for dev in peers:
        pl.semaphore_signal(barrier, inc=1, device_id=dev, device_id_type=MESH_ID)
    pl.semaphore_wait(barrier, len(peers))

    oth_in.wait()
    own_in.wait()
    send(ph, xa.at[0, c, zl], sw_s, sw_r, {"zl": 1 - zl})

    subs = (zl, 1 - zl)

    def to_minus(k, j):
        t = xa.at[k, c, subs[j]]
        u = xa.at[k + 1, c, subs[j]]
        send(t, u, ring_s, ring_r.at[0, k, j], ydev(-1))

    def to_plus(k, j):
        t = xa.at[(NY - k) % NY, c, subs[j]]
        u = xa.at[NY - k - 1, c, subs[j]]
        send(t, u, ring_s, ring_r.at[1, k, j], ydev(1))

    def to_sibling(k, j):
        t = xa.at[k, c, subs[j]]
        send(t, t, sib_s, sib_r.at[k, j], sibling)

    def from_sibling(k, j):
        arrived(xa.at[k, 1 - c, subs[j]], sib_s, sib_r.at[k, j])

    def partial_margin(g, j):
        off, n = GROUPS[g]
        s = subs[j]
        for p in range(off, off + n):
            k, r = FACTORS[p]
            v = dot(xa[k, 0, s], xa[r, 0, c], (((0,), (0,)), ((), ())))
            v = v + dot(xa[k, 1, s], xa[r, 1, c], (((0,), (0,)), ((), ())))
            v = v.astype(BF16)
            xs[2 * s, p] = v[:xrows]
            xs[2 * s + 1, p] = v[xrows:]
        for i in range(2):
            to = 2 * s + i
            d = lax.rem(to - x + NX, NX)
            at = jnp.maximum(d - 1, 0)
            h = copy(xs.at[to, pl.ds(off, n)], xr.at[at, pl.ds(off, n)], x_s, x_r.at[g], {"x": to})

            @pl.when(d > 0)
            def _():
                h.start()

    def sum_over_x(g):
        off, n = GROUPS[g]
        arrived(xr.at[:, pl.ds(off, n)], x_s, x_r.at[g])
        for p in range(off, off + n):
            v = xs[x, p].astype(F32)
            for d in range(1, NX):
                v = v + xr[d - 1, p].astype(F32)
            zs[:, p] = v.astype(BF16).reshape(NZ, zrows, band)
        for d in range(1, NZ):
            t = lax.rem(z + d, NZ)
            send(
                zs.at[t, pl.ds(off, n)], zr.at[d - 1, pl.ds(off, n)],
                z_s, z_r.at[g], zdev(d),
            )

    def sum_over_z(g):
        off, n = GROUPS[g]
        arrived(zr.at[:, pl.ds(off, n)], z_s, z_r.at[g])
        for p in range(off, off + n):
            v = zs[z, p].astype(F32)
            for d in range(1, NZ):
                v = v + zr[d - 1, p].astype(F32)
            v = v * (1.0 / total_rows)
            if p == 0:
                v = v - unit(zrows, band, x * xrows + z * zrows, c * band)
            w = v.astype(BF16)
            if p == FAR:
                dq[...] = w
                send(dq, db.at[p], q_s, q_r, ydev(-2))
            else:
                d32[p] = v
                db[p] = w
                da[p, z, x] = w

    def place_far():
        arrived(db.at[FAR], q_s, q_r)
        da[FAR, z, x] = db[FAR]

    def unit(rows, cols, row0, col0):
        i = lax.broadcasted_iota(jnp.int32, (rows, cols), 0) + row0
        j = lax.broadcasted_iota(jnp.int32, (rows, cols), 1) + col0
        return (i == j).astype(F32)

    for j in range(2):
        if j == 1:
            arrived(xa.at[0, c, 1 - zl], sw_s, sw_r)
        to_minus(0, j)
        to_plus(0, j)
        to_sibling(0, j)
    def ring_step(h, j):
        if h < 4 or j == 0:
            arrived(xa.at[h, c, subs[j]], ring_s, ring_r.at[0, h - 1, j])
            if h < 3 or (h == 3 and j == 0):
                to_minus(h, j)
            to_sibling(h, j)
        if h < 4 or j == 1:
            arrived(xa.at[NY - h, c, subs[j]], ring_s, ring_r.at[1, h - 1, j])
            if h < 3 or (h == 3 and j == 1):
                to_plus(h, j)
            to_sibling(NY - h, j)

    def gather_x(g):
        off, n = GROUPS[g]
        v = da.at[pl.ds(off, n), z, x]
        for d in range(1, NX):
            send(v, v, gx_s, gx_r.at[g // 4], xdev(d))

    def slab(g, i, h):
        off, n = GROUPS[g]
        t = lax.rem(z + (h if i == 0 else NZ - h), NZ)
        return t, pl.ds(off, n)

    def hop_send(g, i, h):
        t, ps = slab(g, i, h - 1)
        v = da.at[ps, t] if h < 4 else da.at[ps, t, pl.ds(2 * i, 2)]
        send(v, v, gz_s, gz_r.at[g // 4, i, h - 1], zdev(-1 if i == 0 else 1))

    def gather_z(g):
        off, n = GROUPS[g]
        arrived(da.at[pl.ds(off, n), z, pl.ds(0, NX - 1)], gx_s, gx_r.at[g // 4])
        for i in range(2):
            hop_send(g, i, 1)

    def hop(g, h):
        for i in range(2):
            t, ps = slab(g, i, h)
            v = da.at[ps, t] if h < 4 else da.at[ps, t, pl.ds(2 * i, 2)]
            arrived(v, gz_s, gz_r.at[g // 4, i, h - 1])
            if h < 4:
                hop_send(g, i, h + 1)

    def near_z(g):
        off, n = GROUPS[g]
        v = da.at[pl.ds(off, n), z, x]
        for d in range(1, NZ):
            send(db.at[pl.ds(off, n)], v, hz_s, hz_r.at[g - 1, d - 1], zdev(d))

    def pieces_x(g, rs):
        off, n = GROUPS[g]
        for r in rs:
            t = lax.rem(z + r, NZ)
            v = da.at[pl.ds(off, n), t, x]
            if r:
                arrived(v, hz_s, hz_r.at[g - 1, NZ - 1 - r])
            for d in (1, 3, 2):
                send(v if r else db.at[pl.ds(off, n)], v, hp_s, hp_r.at[g - 1], xdev(d))

    def pieces_done(g):
        off, n = GROUPS[g]
        arrived(da.at[pl.ds(off, n), :, pl.ds(0, NX - 1)], hp_s, hp_r.at[g - 1])

    PARTS = ((0, 6), (6, 2))

    def rows_part(i):
        off, n = PARTS[i]
        return pl.ds(off, n)

    def left_send(i):
        ps = rows_part(i)
        for k in range(1, NY):
            send(db.at[ps], dj.at[k, c, ps], y_s, y_r, ydev(-k))
        off, n = PARTS[i]
        for p in range(off, off + n):
            dj[0, c, p] = db[p]
        if i == 1:
            send(db, dj.at[0, c], yf_s, yf_r.at[0], sibling)

    def left_pass():
        v = dj.at[pl.ds(1, NY - 1), c]
        arrived(v, y_s, y_r)
        send(v, v, yf_s, yf_r.at[1], sibling)

    def pair_in(h, j):
        from_sibling(h, j)
        from_sibling(NY - h, j)

    ring_step(1, 0)
    from_sibling(0, 0)
    from_sibling(0, 1)
    partial_margin(0, 0)
    partial_margin(0, 1)
    pair_in(1, 0)
    partial_margin(4, 0)
    ring_step(1, 1)
    pair_in(1, 1)
    partial_margin(4, 1)
    sum_over_x(0)
    ring_step(2, 0)
    pair_in(2, 0)
    partial_margin(1, 0)
    sum_over_z(0)
    gather_x(0)
    ring_step(2, 1)
    sum_over_x(4)
    pair_in(2, 1)
    partial_margin(3, 0)
    partial_margin(3, 1)
    partial_margin(1, 1)
    gather_z(0)
    ring_step(3, 0)
    hop(0, 1)
    sum_over_z(4)
    gather_x(4)
    pair_in(3, 0)
    partial_margin(2, 0)
    sum_over_x(3)
    sum_over_x(1)
    hop(0, 2)
    ring_step(3, 1)
    gather_z(4)
    pair_in(3, 1)
    partial_margin(2, 1)
    sum_over_z(3)
    sum_over_z(1)
    near_z(1)
    pieces_x(1, (0,))
    hop(0, 3)
    hop(4, 1)
    sum_over_x(2)
    place_far()
    near_z(3)
    pieces_x(3, (0,))
    left_send(0)
    ring_step(4, 0)
    ring_step(4, 1)
    pieces_x(1, (1, 7, 2, 6))
    hop(4, 2)
    pieces_x(1, (3, 5, 4))
    sum_over_z(2)
    near_z(2)
    pieces_x(2, (0,))
    left_send(1)
    pieces_x(3, (1, 7, 2, 6))
    hop(4, 3)
    pieces_x(3, (3, 5, 4))
    pieces_x(2, (1, 7, 2, 6, 3, 5, 4))
    hop(0, 4)
    hop(4, 4)
    left_pass()
    pieces_done(1)
    pieces_done(3)
    arrived(dj.at[0, 1 - c], yf_s, yf_r.at[0])
    arrived(dj.at[pl.ds(1, NY - 1), 1 - c], yf_s, yf_r.at[1])

    def piece(b, t, u):
        off, n = HALVES[b]
        return ca.at[t, u, pl.ds(off, n)]

    def zpiece(b, u, i, h, far):
        off, n = HALVES[b]
        first = (n + 1) // 2
        t = lax.rem(z + (h if i == 0 else NZ - h), NZ)
        if not far:
            return piece(b, t, u)
        return ca.at[t, u, pl.ds(off, first) if i == 0 else pl.ds(off + first, n - first)]

    def a_send(d, i, h):
        v = zpiece(0, lax.rem(x + NX - d, NX), i, h - 1, h == 4)
        send(v, v, az_s, az_r.at[d, i, h - 1], zdev(-1 if i == 0 else 1))

    def a_hop(d, h):
        for i in range(2):
            v = zpiece(0, lax.rem(x + NX - d, NX), i, h, h == 4)
            arrived(v, az_s, az_r.at[d, i, h - 1])
            if h < 4:
                a_send(d, i, h + 1)

    def b_send(i, h):
        v = zpiece(1, x, i, h - 1, h == 4)
        send(v, v, bz_s, bz_r.at[i, h - 1], zdev(-1 if i == 0 else 1))

    def b_along_x(r):
        v = piece(1, lax.rem(z + r, NZ), x)
        for d in (1, 3, 2):
            send(v, v, bx_s, bx_r, xdev(d))

    def b_hop(h):
        for i in range(2):
            arrived(zpiece(1, x, i, h, h == 4), bz_s, bz_r.at[i, h - 1])
            if h < 4:
                b_send(i, h + 1)
        if h < 4:
            b_along_x(h)
            b_along_x(NZ - h)
        else:
            b_along_x(4)

    def plane_gather(between, b_done):
        for d in (1, 3, 2):
            send(piece(0, z, x), piece(0, z, x), ax_s, ax_r.at[d - 1], xdev(d))
        for i in range(2):
            b_send(i, 1)
        for i in range(2):
            a_send(0, i, 1)
        b_along_x(0)
        b_hop(1)
        for d in (1, 3, 2):
            u = lax.rem(x + NX - d, NX)
            arrived(piece(0, z, u), ax_s, ax_r.at[d - 1])
            for i in range(2):
                a_send(d, i, 1)
        a_hop(0, 1)
        between()
        for h in range(2, 6):
            if h < 5:
                b_hop(h)
            else:
                arrived(ca.at[:, pl.ds(0, NX - 1), pl.ds(*HALVES[1])], bx_s, bx_r)
                b_done()
            for d in (1, 3, 2):
                a_hop(d, h - 1)
            if h < 5:
                a_hop(0, h)

    def rows_of(p, s):
        return jnp.concatenate([ca[:, 2 * s + i, p].reshape(xrows, band) for i in range(2)], axis=0)

    def dev_rows(p, s):
        return jnp.concatenate([da[p, :, 2 * s + i].reshape(xrows, band) for i in range(2)], axis=0)

    acc_sq = [None] * NY
    for k in SLOT:
        if POS[k] == GROUPS[2][0]:
            pieces_done(2)
        left = [dj[k, s].reshape(NY * zrows, band) for s in range(2)]
        part = dot(left[0], dev_rows(POS[k], 0)) + dot(left[1], dev_rows(POS[k], 1))
        for p in range(NY):
            m = POS[(k + SLOT[p]) % NY]
            rows = part[p * zrows : (p + 1) * zrows]
            acc_sq[m] = rows if acc_sq[m] is None else acc_sq[m] + rows
    for p in range(NY):
        v = 0.375 * acc_sq[p] - 0.5 * (db[p].astype(F32) if p == FAR else d32[p])
        if p == 0:
            v = v + unit(zrows, band, x * xrows + z * zrows, c * band)
        ca[z, x, p] = v.astype(BF16)

    kg = lax.rem(x * 2 + zh // 2 - y + NY, NY)
    near = jnp.where(kg == 0, 0, jnp.where(kg <= 2, 2 * kg - 1, 2 * (NY - kg)))
    pg = jnp.where(kg == 3, 6, jnp.where(kg == 4, FAR, jnp.where(kg == 5, 7, near)))

    def mirror(core):
        q = lax.rem(zh, 2) * 2 + core
        return da[pg, :, q].reshape(xrows, band).astype(F32)

    def margin_work():
        from_sibling(4, 0)
        from_sibling(4, 1)
        ms[...] = mirror(1 - c).astype(BF16)
        send(ms, mr, m_s, m_r, sibling)

    home = zl == c
    kept = pl.ds(pl.multiple_of(zl * half, half), half)
    swapped = pl.ds(pl.multiple_of((1 - zl) * half, half), half)
    to_pair = {"zl": 1 - zl}

    def product(part):
        for i, cc in enumerate((1 - c, c)):
            tile = half // 2
            for m in range(2):
                rows = pl.ds(m * tile, tile)
                v = None
                for p in range(HALVES[part][0], sum(HALVES[part])):
                    for s in range(2):
                        w = dot(xa[SLOT[p], cc, s, rows], rows_of(p, s))
                        v = w if v is None else v + w
                if part == 1:
                    acc[i, rows] = v
                    continue
                osb[i, rows] = (acc[i, rows] + v).astype(BF16)
                if i == 0:
                    copy(osb.at[0, rows], rb.at[rows], os_s, os_r, sibling).start()
                else:

                    @pl.when(jnp.logical_not(home))
                    def _():
                        copy(osb.at[1, rows], land.at[rows], oz_s, oz_r, to_pair).start()

        if part == 0:

            @pl.when(home)
            def _():
                o_out[kept, :] = osb[1]

    def first_half():
        arrived(mr, m_s, m_r)
        v = jnp.where(zl == c, mirror(c), mr[...].astype(F32))
        rows0 = (y * 2 + zl) * band
        cols0 = (x * 8 + zh * 2 + c) * xrows
        m_out[...] = v.T + unit(band, xrows, rows0, cols0)
        product(1)

    plane_gather(margin_work, first_half)

    @pl.when(home)
    def _():
        arrived(rb, os_s, os_r)
        copy(rb, land, oz_s, oz_r, to_pair).start()

    product(0)

    low = pl.ds(0, NZ - 1)
    three = pl.ds(0, NX - 1)
    for v, sem in (
        (ph, sw_s),
        (xa.at[pl.ds(0, 7), :, 0], ring_s),
        (xa.at[:, :, 0], sib_s),
        (xr, x_s),
        (zr, z_s),
        (dq, q_s),
        (dj.at[pl.ds(1, NY - 1), 0], y_s),
        (dj.at[:, 0], yf_s),
        (da.at[three, 0, three], gx_s),
        (da.at[three, low], gz_s),
        (da.at[pl.ds(0, 5), low, 0], hz_s),
        (da.at[pl.ds(0, 5), :, three], hp_s),
        (ca.at[0, three, pl.ds(*HALVES[0])], ax_s),
        (ca.at[low, :, pl.ds(*HALVES[0])], az_s),
        (ca.at[low, 0, pl.ds(*HALVES[1])], bz_s),
        (ca.at[:, three, pl.ds(*HALVES[1])], bx_s),
        (ms, m_s),
    ):
        copy(v, v, sem, m_r, sibling).wait_send()

    @pl.when(jnp.logical_not(home))
    def _():
        arrived(rb, os_s, os_r)
        o_out[kept, :] = rb[...]

    arrived(land, oz_s, oz_r)
    o_out[swapped, :] = land[...]

    copy(rb, rb, os_s, os_r, sibling).wait_send()
    copy(rb, rb, oz_s, oz_r, sibling).wait_send()


def shards(total_rows, orbitals):
    rows, band = orbitals.shape
    half = rows // 2
    xrows = 2 * band // NX
    zrows = xrows // NZ
    dma = pltpu.SemaphoreType.DMA
    v = pltpu.VMEM
    scratch = [
        v((NY, 2, 2, half, band), BF16),
        v((half, band), BF16),
        v((NX, NY, xrows, band), BF16),
        v((NX - 1, NY, xrows, band), BF16),
        v((NZ, NY, zrows, band), BF16),
        v((NZ - 1, NY, zrows, band), BF16),
        v((NY, zrows, band), BF16),
        v((NY, zrows, band), F32),
        v((zrows, band), BF16),
        v((NY, 2, NY, zrows, band), BF16),
        v((NY, NZ, NX, zrows, band), BF16),
        v((NZ, NX, NY, zrows, band), BF16),
        v((xrows, band), BF16),
        v((xrows, band), BF16),
        v((2, half, band), F32),
        v((2, half, band), BF16),
        v((half, band), BF16),
        v((half, band), BF16),
        dma((2,)),
        dma, dma,
        dma, dma((2, 4, 2)),
        dma, dma((NY, 2)),
        dma, dma((5,)),
        dma, dma((5,)),
        dma, dma,
        dma, dma,
        dma, dma((2,)),
        dma, dma((2,)),
        dma, dma((2, 2, 4)),
        dma, dma((3, NZ - 1)),
        dma, dma((3,)),
        dma, dma((NX - 1,)),
        dma, dma((NX, 2, 4)),
        dma, dma((2, 4)),
        dma, dma,
        dma, dma,
        dma, dma,
        dma, dma,
    ]

    def body(*refs):
        kernel(total_rows, *refs)

    margin, corrected = pl.pallas_call(
        body,
        out_shape=(v((band, xrows), F32), v((rows, band), BF16)),
        in_specs=[pl.BlockSpec(memory_space=pl.ANY)],
        out_specs=(pl.BlockSpec(memory_space=pltpu.VMEM), pl.BlockSpec(memory_space=pltpu.VMEM)),
        scratch_shapes=scratch,
        compiler_params=pltpu.CompilerParams(
            collective_id=0, has_side_effects=True, vmem_limit_bytes=56 * 1024 * 1024
        ),
    )(orbitals)
    return pl.pallas_call(
        write_out,
        out_shape=(
            jax.ShapeDtypeStruct((band, xrows), F32),
            jax.ShapeDtypeStruct((rows, band), BF16),
        ),
        in_specs=[pl.BlockSpec(memory_space=pltpu.VMEM)] * 2,
        out_specs=(pl.BlockSpec(memory_space=pl.ANY),) * 2,
        scratch_shapes=[dma((2,))],
        compiler_params=pltpu.CompilerParams(vmem_limit_bytes=4 * 1024 * 1024),
    )(margin, corrected)


def write_out(m_ref, o_ref, m_out, o_out, sem):
    copies = [
        pltpu.make_async_copy(m_ref, m_out, sem.at[0]),
        pltpu.make_async_copy(o_ref, o_out, sem.at[1]),
    ]
    for h in copies:
        h.start()
    for h in copies:
        h.wait()


def solution(mesh):
    finer = Mesh(mesh.devices.reshape(NY, 2, NX, NZ // 2, 2), AXES)
    coeffs = ("x", "zh", "c")
    bands = ("y", "zl")

    def run(orbitals):
        total = orbitals.shape[0]
        return jax.shard_map(
            lambda o: shards(total, o),
            mesh=finer,
            in_specs=(P(coeffs, bands),),
            out_specs=(P(bands, coeffs), P(coeffs, bands)),
            check_vma=False,
        )(orbitals)

    return run
```
